32 devices in a mesh: dp: 1 (over z), x: 32 (over y, x, core).
Axes of the slice: x: 4, y: 4, z: 1, core: 2. Of those that a mesh axis runs over, the one named last changes fastest.
The devices are a block of a 4x4x8 slice.
Arguments:
- c_raw: bfloat16 [512, 1024, 512], P('dp', 'x')
- k_raw: bfloat16 [512, 1024, 64], P('dp', 'x')
- norm_gain: bfloat16 [512], replicated
- rope_cos: float32 [1024, 32], P('x')
- rope_sin: float32 [1024, 32], P('x')
- seq_lens: int32 [512], P('dp')
- q_lat: bfloat16 [512, 16, 512], P(('dp', 'x'))
- q_rope: bfloat16 [512, 16, 64], P(('dp', 'x'))
Outputs:
- output 1: bfloat16 [512, 1024, 512], P(('dp', 'x'))
- output 2: bfloat16 [512, 1024, 64], P(('dp', 'x'))
- output 3: bfloat16 [512, 16, 512], P(('dp', 'x'))
All inputs are finite; a program needn't handle non-finite values.
Results may differ from the reference program's by a relative error of at most 0.00590157.
Values are sent between devices in bfloat16 or wider.
A program may use at most 768 MiB of HBM per device.

```python
import jax
import jax.numpy as jnp
from jax import lax

REQUESTS = 512
SEQ_LEN = 1024
KV_RANK = 512
ROPE_DIM = 64
NUM_HEADS = 16

NORM_EPS = 1e-6
ATTN_SCALE = (KV_RANK + ROPE_DIM) ** -0.5


def setup_inputs(seed: int = 0, part: int = 0) -> dict:
    part_key = jax.random.fold_in(jax.random.key(seed), part)
    keys = jax.random.split(part_key, 8)
    shared = jax.random.split(jax.random.key(seed + 1), 2)
    row_scale = jnp.exp(0.5 * jax.random.normal(keys[0], (REQUESTS, SEQ_LEN, 1), jnp.float32))
    c_raw = (jax.random.normal(keys[1], (REQUESTS, SEQ_LEN, KV_RANK), jnp.float32) * row_scale).astype(jnp.bfloat16)
    k_raw = jax.random.normal(keys[2], (REQUESTS, SEQ_LEN, ROPE_DIM), jnp.float32).astype(jnp.bfloat16)
    norm_gain = (1.0 + 0.3 * jax.random.normal(shared[0], (KV_RANK,), jnp.float32)).astype(jnp.bfloat16)
    half_dim = ROPE_DIM // 2
    log_base = jax.random.uniform(shared[1], (), jnp.float32, 9.0, 14.0)
    inv_freq = jnp.exp(-log_base * (2.0 * jnp.arange(half_dim, dtype=jnp.float32) / ROPE_DIM))
    angles = jnp.arange(SEQ_LEN, dtype=jnp.float32)[:, None] * inv_freq[None, :]
    seq_lens = jax.random.randint(keys[3], (REQUESTS,), SEQ_LEN // 8, SEQ_LEN + 1)
    full_index = jax.random.randint(keys[4], (), 0, REQUESTS)
    short_offset = jax.random.randint(keys[5], (), 1, REQUESTS)
    seq_lens = seq_lens.at[full_index].set(SEQ_LEN)
    seq_lens = seq_lens.at[(full_index + short_offset) % REQUESTS].set(SEQ_LEN // 8)
    q_lat = (1.3 * jax.random.normal(keys[6], (REQUESTS, NUM_HEADS, KV_RANK), jnp.float32)).astype(jnp.bfloat16)
    q_rope = (3.0 * jax.random.normal(keys[7], (REQUESTS, NUM_HEADS, ROPE_DIM), jnp.float32)).astype(jnp.bfloat16)
    return {"c_raw": c_raw, "k_raw": k_raw, "norm_gain": norm_gain, "rope_cos": jnp.cos(angles), "rope_sin": jnp.sin(angles), "seq_lens": seq_lens.astype(jnp.int32), "q_lat": q_lat, "q_rope": q_rope}


def reference(c_raw, k_raw, norm_gain, rope_cos, rope_sin, seq_lens, q_lat, q_rope):
    positions = jnp.arange(SEQ_LEN)
    half_dim = ROPE_DIM // 2
    gain = norm_gain.astype(jnp.float32)

    def one_request(operands):
        c_row, k_row, length, lat_row, rope_row = operands
        valid = positions < length
        lat_f32 = c_row.astype(jnp.float32)
        inv_rms = lax.rsqrt(jnp.mean(lat_f32 * lat_f32, axis=-1, keepdims=True) + NORM_EPS)
        c_norm = jnp.where(valid[:, None], lat_f32 * inv_rms * gain, 0.0).astype(jnp.bfloat16)
        key_f32 = k_row.astype(jnp.float32)
        key_lo = key_f32[:, :half_dim]
        key_hi = key_f32[:, half_dim:]
        rotated = jnp.concatenate([key_lo * rope_cos - key_hi * rope_sin, key_hi * rope_cos + key_lo * rope_sin], axis=-1)
        k_rope = jnp.where(valid[:, None], rotated, 0.0).astype(jnp.bfloat16)
        scores = jnp.dot(lat_row, c_norm.T, preferred_element_type=jnp.float32) + jnp.dot(rope_row, k_rope.T, preferred_element_type=jnp.float32)
        scores = jnp.where(valid[None, :], scores * ATTN_SCALE, -1e30)
        weights = jnp.exp(scores - jnp.max(scores, axis=-1, keepdims=True))
        out_row = jnp.dot(weights, c_norm.astype(jnp.float32)) / jnp.sum(weights, axis=-1, keepdims=True)
        return c_norm, k_rope, out_row.astype(jnp.bfloat16)

    c_cache, kr_cache, o_lat = lax.map(one_request, (c_raw, k_raw, seq_lens, q_lat, q_rope))
    return (c_cache, kr_cache, o_lat)
```

```python
import jax
import jax.numpy as jnp
from jax import lax
from jax.experimental import pallas as pl
from jax.experimental.pallas import tpu as pltpu
from jax.sharding import PartitionSpec as P

NORM_EPS = 1e-6
MESH = pl.DeviceIdType.MESH
MIB = 2**20

OFFSETS = ((2, 2), (1, 1), (3, 3), (1, 3), (3, 1), (1, 2), (3, 0), (3, 2), (1, 0), (2, 1), (0, 3), (2, 3), (0, 1), (2, 0), (0, 2), (0, 0))
SIDE = 4
CORES = 2


def table(values, index):
    out = jnp.int32(values[0])
    for place, value in enumerate(values[1:], 1):
        out = jnp.where(index == place, jnp.int32(value), out)
    return out


def chip_at(me, dx, dy):
    chip = me // CORES
    return lax.rem(chip // SIDE + dy, SIDE) * SIDE + lax.rem(lax.rem(chip, SIDE) + dx, SIDE)


def exchange_kernel(lens_s, c_raw, k_raw, gain, cos, sin, lens_v, c_out, k_out, raw, send_c, k_in, k_rows, send_k, raw_sem, k_sem, c_send, c_recv, k_send, k_recv):
    me = lax.axis_index("x")
    group = lax.axis_index("dp")
    core = lax.rem(me, CORES)
    n_dev = SIDE * SIDE * CORES
    n_off = len(OFFSETS)
    seq_local = c_raw.shape[1]
    req_local = c_out.shape[0]
    half = cos.shape[1]
    first_pos = me * seq_local
    pair_req = CORES * req_local
    dxs = [o[0] for o in OFFSETS]
    dys = [o[1] for o in OFFSETS]

    barrier = pltpu.get_barrier_semaphore()

    def greet(step, carry):
        pl.semaphore_signal(barrier, inc=1, device_id=(group, lax.rem(me + step, n_dev)), device_id_type=MESH)
        return carry

    lax.fori_loop(1, n_dev, greet, 0)

    def chip_of(o):
        return chip_at(me, table(dxs, o), table(dys, o))

    def load(o, slot):
        return pltpu.make_async_copy(c_raw.at[pl.ds(chip_of(o) * pair_req, pair_req)], raw.at[slot], raw_sem.at[slot])

    def norm_one(o, chip, slot, row, store):
        length = lens_s[chip * pair_req + row]
        x = raw[slot, row].astype(jnp.float32)
        inv = lax.rsqrt(jnp.mean(x * x, axis=-1, keepdims=True) + NORM_EPS)
        valid = first_pos + lax.broadcasted_iota(jnp.int32, inv.shape, 0) < length
        y = x * inv * gain[...].astype(jnp.float32)
        store(jnp.where(valid, y, 0.0).astype(jnp.bfloat16))

    def c_copy(o, dc):
        chip = chip_of(o)
        there = lax.rem(core + dc, CORES)
        return pltpu.make_async_remote_copy(
            send_c.at[o, pl.ds(there * req_local, req_local)],
            c_out.at[:, pl.ds(pl.multiple_of(first_pos, 32), seq_local), :],
            c_send.at[o, dc],
            c_recv.at[o, dc],
            device_id=(group, chip * CORES + there),
            device_id_type=MESH,
        )

    def k_copy(o, dc):
        chip = chip_of(o)
        there = lax.rem(core + dc, CORES)
        dest = chip * CORES + there
        return pltpu.make_async_remote_copy(
            send_k.at[pl.ds(dest * req_local, req_local)],
            k_out.at[:, pl.ds(pl.multiple_of(me * (seq_local // 2), 16), seq_local // 2), :],
            k_send.at[o, dc],
            k_recv.at[o, dc],
            device_id=(group, dest),
            device_id_type=MESH,
        )

    def norm_chip(o, slot):
        chip = chip_of(o)

        def body(row, carry):
            def store(y):
                send_c[o, row] = y

            norm_one(o, chip, slot, row, store)
            return carry

        lax.fori_loop(0, pair_req, body, 0, unroll=4)

    k_load = pltpu.make_async_copy(k_raw, k_in, k_sem)
    load(0, 0).start()
    k_load.start()
    load(1, 1).start()
    load(0, 0).wait()
    norm_chip(0, 0)
    load(2, 0).start()

    k_load.wait()
    cos_t = cos[...].T
    sin_t = sin[...].T
    pairs = seq_local // 2
    lane_valid = lens_v[...]

    for pair in range(pairs):
        pieces = []
        for pos in (pair, pair + pairs):
            lo = k_in[pos, :half, :].astype(jnp.float32)
            hi = k_in[pos, half:, :].astype(jnp.float32)
            c = cos_t[:, pos : pos + 1]
            s = sin_t[:, pos : pos + 1]
            keep = first_pos + pos < lane_valid
            pieces.append(jnp.where(keep, lo * c - hi * s, 0.0))
            pieces.append(jnp.where(keep, hi * c + lo * s, 0.0))
        both = jnp.concatenate(pieces, axis=0)
        k_rows[pl.ds(pair, k_rows.shape[0] // pairs, stride=pairs), :] = both.T

    def pack(step, carry):
        rows = k_rows[pl.ds(pl.multiple_of(step * 256, 256), 256), :].astype(jnp.bfloat16)
        send_k[pl.ds(step * 16, 16)] = rows.reshape(16, 16, 128)
        return carry

    lax.fori_loop(0, n_dev, pack, 0)

    pl.semaphore_wait(barrier, n_dev - 1)
    c_copy(0, 0).start()
    c_copy(0, 1).start()

    def start_k(o, carry):
        k_copy(o, 0).start()
        k_copy(o, 1).start()
        return carry

    lax.fori_loop(0, n_off - 1, start_k, 0)
    k_copy(n_off - 1, 1).start()
    k_out[:, pl.ds(pl.multiple_of(me * pairs, 16), pairs), :] = send_k[pl.ds(me * req_local, req_local)]

    def step(o, carry):
        slot = lax.rem(o, 2)
        load(o, slot).wait()
        norm_chip(o, slot)

        @pl.when(o + 2 < n_off)
        def _():
            load(o + 2, slot).start()

        c_copy(o, 0).start()
        c_copy(o, 1).start()
        return carry

    lax.fori_loop(1, n_off - 1, step, 0)

    last = n_off - 1
    slot = last % 2
    load(last, slot).wait()
    norm_chip(last, slot)
    c_copy(last, 1).start()
    c_out[:, pl.ds(pl.multiple_of(first_pos, 32), seq_local), :] = send_c[last, pl.ds(core * req_local, req_local)]

    def finish(o, carry):
        for copy in (c_copy, k_copy):
            for dc in range(CORES):
                copy(o, dc).wait_send()
                copy(o, dc).wait_recv()
        return carry

    lax.fori_loop(0, n_off - 1, finish, 0)
    for copy in (c_copy, k_copy):
        copy(last, 1).wait_send()
        copy(last, 1).wait_recv()


def attend_kernel(lens_s, c_in, k_in, q_lat, q_rope, c_out, k_out, o_out, k_turned, c_sem, k_sem):
    me = lax.axis_index("x")
    n_req, seq, width = c_in.shape
    rope = q_rope.shape[-1]
    heads = q_lat.shape[1]
    scale = (width + rope) ** -0.5
    pairs = 16

    def c_copy(r):
        return pltpu.make_async_copy(c_in.at[r], c_out.at[r], c_sem.at[r])

    def k_copy(r):
        return pltpu.make_async_copy(k_turned.at[r], k_out.at[r], k_sem.at[r])

    def start(r, carry):
        c_copy(r).start()
        return carry

    lax.fori_loop(0, n_req, start, 0)
    eye = (lax.broadcasted_iota(jnp.int32, (rope, 2 * rope), 0) == lax.rem(lax.broadcasted_iota(jnp.int32, (rope, 2 * rope), 1), rope)).astype(jnp.bfloat16)
    low_lane = lax.broadcasted_iota(jnp.int32, (1, 1, 2 * rope), 2) < rope

    def attend(r, carry):
        length = lens_s[me * n_req + r]
        both = k_in[r].reshape(seq // (2 * pairs), pairs, 2 * rope)
        zero = jnp.zeros_like(both)
        rows = jnp.concatenate([jnp.where(low_lane, both, zero)[:, None], jnp.where(low_lane, zero, both)[:, None]], axis=1).reshape(seq, 2 * rope)
        qr = q_rope[r]
        left = jnp.concatenate([jnp.concatenate([qr, qr], axis=1), eye], axis=0)
        turned = lax.dot_general(left, rows, (((1,), (1,)), ((), ())), preferred_element_type=jnp.float32)
        k_turned[r] = turned[heads:].astype(jnp.bfloat16)
        k_copy(r).start()
        c_req = c_in[r]
        scores = lax.dot_general(q_lat[r], c_req, (((1,), (1,)), ((), ())), preferred_element_type=jnp.float32)
        scores = (scores + turned[:heads]) * scale
        valid = lax.broadcasted_iota(jnp.int32, scores.shape, 1) < length
        scores = jnp.where(valid, scores, -1e30)
        weights = jnp.exp(scores - jnp.max(scores, axis=-1, keepdims=True))
        total = jnp.sum(weights, axis=-1, keepdims=True)
        mixed = jnp.dot(weights.astype(jnp.bfloat16), c_req, preferred_element_type=jnp.float32)
        o_out[r] = (mixed / total).astype(jnp.bfloat16)
        return carry

    lax.fori_loop(0, n_req, attend, 0)

    def finish(r, carry):
        c_copy(r).wait()
        k_copy(r).wait()
        return carry

    lax.fori_loop(0, n_req, finish, 0)


def solution(mesh):
    seq_spec = P("dp", "x", None)
    req_spec = P(("dp", "x"), None, None)
    vmem = pl.BlockSpec(memory_space=pltpu.VMEM)
    smem = pl.BlockSpec(memory_space=pltpu.SMEM)
    anywhere = pl.BlockSpec(memory_space=pl.ANY)

    def local_step(c_raw, k_raw, norm_gain, rope_cos, rope_sin, seq_lens, q_lat, q_rope):
        n_all, seq_local, width = c_raw.shape
        rope = k_raw.shape[-1]
        req_local, heads, _ = q_lat.shape
        n_dev = n_all // req_local
        seq = n_dev * seq_local
        pairs = seq_local // 2
        n_off = len(OFFSETS)
        lens_row = seq_lens.reshape(1, n_all)
        c_here, k_here = pl.pallas_call(
            exchange_kernel,
            out_shape=(pltpu.VMEM((req_local, seq, width), jnp.bfloat16), pltpu.VMEM((req_local, seq // 2, 2 * rope), jnp.bfloat16)),
            in_specs=[smem, anywhere, anywhere, vmem, vmem, vmem, vmem],
            out_specs=(vmem, vmem),
            scratch_shapes=[
                pltpu.VMEM((2, CORES * req_local, seq_local, width), jnp.bfloat16),
                pltpu.VMEM((n_off, CORES * req_local, seq_local, width), jnp.bfloat16),
                pltpu.VMEM((seq_local, rope, n_all), jnp.bfloat16),
                pltpu.VMEM((n_all * pairs, 2 * rope), jnp.float32),
                pltpu.VMEM((n_all, pairs, 2 * rope), jnp.bfloat16),
                pltpu.SemaphoreType.DMA((2,)),
                pltpu.SemaphoreType.DMA,
                pltpu.SemaphoreType.DMA((n_off, CORES)),
                pltpu.SemaphoreType.DMA((n_off, CORES)),
                pltpu.SemaphoreType.DMA((n_off, CORES)),
                pltpu.SemaphoreType.DMA((n_off, CORES)),
            ],
            compiler_params=pltpu.CompilerParams(collective_id=0, has_side_effects=True, vmem_limit_bytes=34 * MIB),
            name="exchange",
        )(seq_lens, c_raw, jnp.transpose(k_raw, (1, 2, 0)), norm_gain.reshape(1, width), rope_cos, rope_sin, lens_row)
        c_cache, k_turned, o_lat = pl.pallas_call(
            attend_kernel,
            out_shape=(
                jax.ShapeDtypeStruct((req_local, seq, width), jnp.bfloat16),
                jax.ShapeDtypeStruct((req_local, rope, seq), jnp.bfloat16),
                jax.ShapeDtypeStruct((req_local, heads, width), jnp.bfloat16),
            ),
            in_specs=[smem, vmem, vmem, vmem, vmem],
            out_specs=(anywhere, anywhere, vmem),
            scratch_shapes=[
                pltpu.VMEM((req_local, rope, seq), jnp.bfloat16),
                pltpu.SemaphoreType.DMA((req_local,)),
                pltpu.SemaphoreType.DMA((req_local,)),
            ],
            compiler_params=pltpu.CompilerParams(vmem_limit_bytes=16 * MIB),
            name="attend",
        )(seq_lens, c_here, k_here, q_lat, q_rope)
        return c_cache, jnp.transpose(k_turned, (0, 2, 1)), o_lat

    return jax.shard_map(local_step, mesh=mesh, in_specs=(seq_spec, seq_spec, P(None), P("x", None), P("x", None), P("dp"), req_spec, req_spec), out_specs=(req_spec, req_spec, req_spec), check_vma=False)
```

```python
import functools
import math

import jax
import jax.numpy as jnp
from jax import lax
from jax.experimental import pallas as pl
from jax.experimental.pallas import tpu as pltpu
from jax.sharding import PartitionSpec as P

NORM_EPS = 1e-6
MASKED = -1e30
MESH = pl.DeviceIdType.MESH
MIB = 2**20
CORES = 2
TOGETHER = 8

STAGES = (
    ((2, 2), (0, 0)),
    ((1, 1), (-1, -1)),
    ((1, -1), (-1, 1)),
    ((1, 2), (-1, 0)),
    ((-1, 2), (1, 0)),
    ((2, 1), (0, -1)),
    ((2, -1), (0, 1)),
    ((2, 0), (0, 2)),
)
OFFSETS = tuple(offset for stage in STAGES for offset in stage)
OWN = OFFSETS.index((0, 0))
NT = (((1,), (1,)), ((), ()))


def table(values, index):
    if isinstance(index, int):
        return values[index]
    out = jnp.int32(values[0])
    for place, value in enumerate(values[1:], 1):
        out = jnp.where(index == place, jnp.int32(value), out)
    return out


def chip_at(me, side, place, sign=1):
    chip = me // CORES
    dx = table([(sign * dx) % side for dx, _ in OFFSETS], place)
    dy = table([(sign * dy) % side for _, dy in OFFSETS], place)
    return lax.rem(chip // side + dy, side) * side + lax.rem(lax.rem(chip, side) + dx, side)


def stack_keys(pairs_rows):
    lanes = pairs_rows.shape[-1]
    low = lax.broadcasted_iota(jnp.int32, (1, 1, lanes), 2) < lanes // 2
    zero = jnp.zeros_like(pairs_rows)
    split = [jnp.where(low, pairs_rows, zero)[:, None], jnp.where(low, zero, pairs_rows)[:, None]]
    return jnp.concatenate(split, axis=1).reshape(-1, lanes)


def attend_stage(chips, lengths, queries, c_ref, k_ref, requests, seq_local, states):
    span = CORES * seq_local
    starts = [pl.multiple_of(chip * span, span) for chip in chips]
    rows = [jnp.concatenate([c_ref[r, pl.ds(start, span), :] for start in starts], axis=0) for r in requests]
    keys = [jnp.concatenate([stack_keys(k_ref[pl.ds(chip * CORES, CORES), r]) for chip in chips], axis=0) for r in requests]
    scale = (rows[0].shape[-1] + keys[0].shape[-1] // 2) ** -0.5
    scores = [lax.dot_general(q, jnp.concatenate([row, key], axis=1), NT, preferred_element_type=jnp.float32) for q, row, key in zip(queries, rows, keys)]
    lane = lax.broadcasted_iota(jnp.int32, scores[0].shape, 1)
    position = jnp.where(lane < span, starts[0] + lane, starts[1] - span + lane)
    scores = [jnp.where(position < length, score * scale, MASKED) for score, length in zip(scores, lengths)]
    tops = [jnp.maximum(state[0], jnp.max(score, axis=-1, keepdims=True)) for state, score in zip(states, scores)]
    keeps = [jnp.exp(state[0] - top) for state, top in zip(states, tops)]
    weights = [jnp.exp(score - top) for score, top in zip(scores, tops)]
    added = [jnp.dot(weight.astype(jnp.bfloat16), row, preferred_element_type=jnp.float32) for weight, row in zip(weights, rows)]
    out = []
    for (_, total, mixed), top, keep, weight, add in zip(states, tops, keeps, weights, added):
        wide_keep = jnp.concatenate([keep] * (mixed.shape[-1] // keep.shape[-1]), axis=1)
        out.append((top, total * keep + weight, mixed * wide_keep + add))
    return out


def exchange_kernel(
    side, lens_h, c_raw, k_raw, gain_h, cos_h, sin_h, q_lat_h, q_rope_h,
    c_out, k_out, top_out, total_out, mixed_out,
    lens_s, lens_v, gain, cos, sin, q_lat, q_rope, raw, send_c, k_in, k_rows, send_k,
    small_sem, raw_sem, k_sem, c_send, c_recv, k_send, k_recv,
):
    me = lax.axis_index("x")
    group = lax.axis_index("dp")
    core = lax.rem(me, CORES)
    n_dev = side * side * CORES
    n_off = len(OFFSETS)
    seq_local = c_raw.shape[1]
    req_local, heads, _ = q_lat.shape
    pair_req = CORES * req_local
    half = cos.shape[1]
    pairs = seq_local // 2
    first_pos = me * seq_local

    barrier = pltpu.get_barrier_semaphore()

    def greet(step, carry):
        pl.semaphore_signal(barrier, inc=1, device_id=(group, lax.rem(me + step, n_dev)), device_id_type=MESH)
        return carry

    lax.fori_loop(1, n_dev, greet, 0)

    def load(o, slot):
        return pltpu.make_async_copy(c_raw.at[pl.ds(chip_at(me, side, o) * pair_req, pair_req)], raw.at[slot], raw_sem.at[slot])

    def c_copy(o, dc):
        chip = chip_at(me, side, o)
        there = lax.rem(core + dc, CORES)
        return pltpu.make_async_remote_copy(
            send_c.at[o, pl.ds(there * req_local, req_local)],
            c_out.at[:, pl.ds(pl.multiple_of(first_pos, 32), seq_local), :],
            c_send.at[o, dc],
            c_recv.at[o, dc],
            device_id=(group, chip * CORES + there),
            device_id_type=MESH,
        )

    def k_copy(o, dc):
        chip = chip_at(me, side, o)
        there = lax.rem(core + dc, CORES)
        dest = chip * CORES + there
        return pltpu.make_async_remote_copy(
            send_k.at[pl.ds(dest * req_local, req_local)],
            k_out.at[me],
            k_send.at[o, dc],
            k_recv.at[o, dc],
            device_id=(group, dest),
            device_id_type=MESH,
        )

    def norm_chip(o, slot):
        first = chip_at(me, side, o) * pair_req
        scale = gain[...].astype(jnp.float32).reshape(1, gain.shape[0])

        def body(row, carry):
            length = lens_s[0, first + row]
            x = raw[slot, row].astype(jnp.float32)
            inv = lax.rsqrt(jnp.mean(x * x, axis=-1, keepdims=True) + NORM_EPS)
            valid = first_pos + lax.broadcasted_iota(jnp.int32, inv.shape, 0) < length
            send_c[o, row] = jnp.where(valid, x * inv * scale, 0.0).astype(jnp.bfloat16)
            return carry

        lax.fori_loop(0, pair_req, body, 0, unroll=4)

    small = [
        pltpu.make_async_copy(src, dst, small_sem.at[i])
        for i, (src, dst) in enumerate(((lens_h, lens_s), (gain_h, gain), (lens_h, lens_v), (cos_h, cos), (sin_h, sin), (q_lat_h, q_lat), (q_rope_h, q_rope)))
    ]
    k_load = pltpu.make_async_copy(k_raw, k_in, k_sem)
    load(0, 0).start()
    small[0].start()
    small[1].start()
    load(1, 1).start()
    k_load.start()
    for copy in small[2:]:
        copy.start()
    small[0].wait()
    small[1].wait()
    load(0, 0).wait()
    norm_chip(0, 0)
    load(2, 0).start()
    pl.semaphore_wait(barrier, n_dev - 1)
    c_copy(0, 0).start()
    c_copy(0, 1).start()

    for copy in small[2:]:
        copy.wait()
    k_load.wait()
    cos_t = cos[...].T
    sin_t = sin[...].T
    for pair in range(pairs):
        pieces = []
        for pos in (pair, pair + pairs):
            lo = k_in[pos, :half, :].astype(jnp.float32)
            hi = k_in[pos, half:, :].astype(jnp.float32)
            c = cos_t[:, pos : pos + 1]
            s = sin_t[:, pos : pos + 1]
            keep = first_pos + pos < lens_v[...]
            pieces.append(jnp.where(keep, lo * c - hi * s, 0.0))
            pieces.append(jnp.where(keep, hi * c + lo * s, 0.0))
        k_rows[pl.ds(pair, k_rows.shape[0] // pairs, stride=pairs), :] = jnp.concatenate(pieces, axis=0).T

    def pack(step, carry):
        rows = k_rows[pl.ds(pl.multiple_of(step * req_local * pairs, 256), req_local * pairs), :].astype(jnp.bfloat16)
        send_k[pl.ds(step * req_local, req_local)] = rows.reshape(req_local, pairs, k_rows.shape[1])
        return carry

    lax.fori_loop(0, n_dev, pack, 0)

    def start_k(o):
        @pl.when(o != OWN)
        def _():
            k_copy(o, 0).start()

        k_copy(o, 1).start()

    start_k(jnp.int32(0))
    k_out[me] = send_k[pl.ds(me * req_local, req_local)]

    def produce(o, carry):
        slot = lax.rem(o, 2)
        load(o, slot).wait()
        norm_chip(o, slot)

        @pl.when(o + 2 < n_off)
        def _():
            load(o + 2, slot).start()

        @pl.when(o != OWN)
        def _():
            c_copy(o, 0).start()

        c_copy(o, 1).start()

        start_k(o)
        return carry

    lax.fori_loop(1, n_off, produce, 0)
    c_out[:, pl.ds(pl.multiple_of(first_pos, 32), seq_local), :] = send_c[OWN, pl.ds(core * req_local, req_local)]

    def clear(r, carry):
        top_out[r] = jnp.full(top_out.shape[1:], MASKED, jnp.float32)
        total_out[r] = jnp.zeros(total_out.shape[1:], jnp.float32)
        mixed_out[r] = jnp.zeros(mixed_out.shape[1:], jnp.float32)
        return carry

    lax.fori_loop(0, req_local, clear, 0)

    def arrived(o):
        @pl.when(o != OWN)
        def _():
            c_copy(o, 0).wait_recv()
            k_copy(o, 0).wait_recv()

        c_copy(o, 1).wait_recv()
        k_copy(o, 1).wait_recv()

    def attend(stage, carry):
        chips = [chip_at(me, side, 2 * stage + i, -1) for i in range(2)]
        arrived(2 * stage)
        arrived(2 * stage + 1)

        def some(step, carry):
            requests = [step * TOGETHER + i for i in range(TOGETHER)]
            queries = [jnp.concatenate([q_lat[r], q_rope[r], q_rope[r]], axis=1) for r in requests]
            lengths = [lens_s[0, me * req_local + r] for r in requests]
            states = [(top_out[r], total_out[r], mixed_out[r]) for r in requests]
            states = attend_stage(chips, lengths, queries, c_out, k_out, requests, seq_local, states)
            for r, state in zip(requests, states):
                top_out[r], total_out[r], mixed_out[r] = state
            return carry

        lax.fori_loop(0, req_local // TOGETHER, some, 0)
        return carry

    lax.fori_loop(0, len(STAGES) - 1, attend, 0)
    arrived(jnp.int32(n_off - 2))
    arrived(jnp.int32(n_off - 1))

    def sent(o, carry):
        for copy in (c_copy, k_copy):

            @pl.when(o != OWN)
            def _():
                copy(o, 0).wait_send()

            copy(o, 1).wait_send()
        return carry

    lax.fori_loop(0, n_off, sent, 0)


def finish_kernel(side, lens_s, c_in, k_in, top, total, mixed, q_lat_h, q_rope_h, c_cache, k_cache, o_out, turned, q_lat, q_rope, c_sem, k_sem, q_sem):
    me = lax.axis_index("x")
    n_req, seq, _ = c_in.shape
    seq_local = seq // (side * side * CORES)
    n_off = len(OFFSETS)

    def c_copy(r):
        return pltpu.make_async_copy(c_in.at[r], c_cache.at[r], c_sem.at[r])

    q_copies = [pltpu.make_async_copy(src, dst, q_sem.at[i]) for i, (src, dst) in enumerate(((q_lat_h, q_lat), (q_rope_h, q_rope)))]
    for copy in q_copies:
        copy.start()

    def start(r, carry):
        c_copy(r).start()
        return carry

    lax.fori_loop(0, n_req, start, 0)
    k_copy = pltpu.make_async_copy(turned, k_cache, k_sem)
    rope = turned.shape[1]
    shape = (rope, 2 * rope)
    eye = (lax.broadcasted_iota(jnp.int32, shape, 0) == lax.rem(lax.broadcasted_iota(jnp.int32, shape, 1), rope)).astype(jnp.bfloat16)

    def turn(step, carry):
        requests = [step * 4 + i for i in range(4)]
        results = [lax.dot_general(eye, stack_keys(k_in[:, r]), NT, preferred_element_type=jnp.float32) for r in requests]
        for r, result in zip(requests, results):
            turned[r] = result.astype(jnp.bfloat16)
        return carry

    lax.fori_loop(0, n_req // 4, turn, 0)
    k_copy.start()
    for copy in q_copies:
        copy.wait()
    chips = [chip_at(me, side, n_off - 2 + i, -1) for i in range(2)]

    def some(step, carry):
        requests = [step * TOGETHER + i for i in range(TOGETHER)]
        queries = [jnp.concatenate([q_lat[r], q_rope[r], q_rope[r]], axis=1) for r in requests]
        lengths = [lens_s[me * n_req + r] for r in requests]
        states = [(top[r], total[r], mixed[r]) for r in requests]
        states = attend_stage(chips, lengths, queries, c_in, k_in, requests, seq_local, states)
        for r, (_, weights, values) in zip(requests, states):
            o_out[r] = (values / jnp.sum(weights, axis=-1, keepdims=True)).astype(jnp.bfloat16)
        return carry

    lax.fori_loop(0, n_req // TOGETHER, some, 0)

    def finish(r, carry):
        c_copy(r).wait()
        return carry

    lax.fori_loop(0, n_req, finish, 0)
    k_copy.wait()


def solution(mesh):
    seq_spec = P("dp", "x", None)
    req_spec = P(("dp", "x"), None, None)
    vmem = pl.BlockSpec(memory_space=pltpu.VMEM)
    smem = pl.BlockSpec(memory_space=pltpu.SMEM)
    anywhere = pl.BlockSpec(memory_space=pl.ANY)
    n_dev = mesh.shape["x"]
    side = math.isqrt(n_dev // CORES)

    def local_step(c_raw, k_raw, norm_gain, rope_cos, rope_sin, seq_lens, q_lat, q_rope):
        n_all, seq_local, width = c_raw.shape
        rope = k_raw.shape[-1]
        req_local, heads, _ = q_lat.shape
        seq = n_dev * seq_local
        pairs = seq_local // 2
        n_off = len(OFFSETS)
        lanes = 2 * CORES * seq_local
        state = pltpu.VMEM((req_local, heads, lanes), jnp.float32)
        received = pl.pallas_call(
            functools.partial(exchange_kernel, side),
            out_shape=(
                pltpu.VMEM((req_local, seq, width), jnp.bfloat16),
                pltpu.VMEM((n_dev, req_local, pairs, 2 * rope), jnp.bfloat16),
                state,
                state,
                pltpu.VMEM((req_local, heads, width), jnp.float32),
            ),
            in_specs=[anywhere] * 8,
            out_specs=(vmem,) * 5,
            scratch_shapes=[
                pltpu.SMEM((1, n_all), jnp.int32),
                pltpu.VMEM((1, n_all), jnp.int32),
                pltpu.VMEM((width,), jnp.bfloat16),
                pltpu.VMEM(rope_cos.shape, jnp.float32),
                pltpu.VMEM(rope_sin.shape, jnp.float32),
                pltpu.VMEM(q_lat.shape, jnp.bfloat16),
                pltpu.VMEM(q_rope.shape, jnp.bfloat16),
                pltpu.VMEM((2, CORES * req_local, seq_local, width), jnp.bfloat16),
                pltpu.VMEM((n_off, CORES * req_local, seq_local, width), jnp.bfloat16),
                pltpu.VMEM((seq_local, rope, n_all), jnp.bfloat16),
                pltpu.VMEM((n_all * pairs, 2 * rope), jnp.float32),
                pltpu.VMEM((n_all, pairs, 2 * rope), jnp.bfloat16),
                pltpu.SemaphoreType.DMA((7,)),
                pltpu.SemaphoreType.DMA((2,)),
                pltpu.SemaphoreType.DMA,
                pltpu.SemaphoreType.DMA((n_off, CORES)),
                pltpu.SemaphoreType.DMA((n_off, CORES)),
                pltpu.SemaphoreType.DMA((n_off, CORES)),
                pltpu.SemaphoreType.DMA((n_off, CORES)),
            ],
            compiler_params=pltpu.CompilerParams(collective_id=0, has_side_effects=True, vmem_limit_bytes=42 * MIB),
            name="exchange",
        )(seq_lens.reshape(1, n_all), c_raw, jnp.transpose(k_raw, (1, 2, 0)), norm_gain, rope_cos, rope_sin, q_lat, q_rope)
        c_cache, k_turned, o_lat = pl.pallas_call(
            functools.partial(finish_kernel, side),
            out_shape=(
                jax.ShapeDtypeStruct((req_local, seq, width), jnp.bfloat16),
                jax.ShapeDtypeStruct((req_local, rope, seq), jnp.bfloat16),
                jax.ShapeDtypeStruct((req_local, heads, width), jnp.bfloat16),
            ),
            in_specs=[smem] + [vmem] * 5 + [anywhere] * 2,
            out_specs=(anywhere, anywhere, vmem),
            scratch_shapes=[
                pltpu.VMEM((req_local, rope, seq), jnp.bfloat16),
                pltpu.VMEM(q_lat.shape, jnp.bfloat16),
                pltpu.VMEM(q_rope.shape, jnp.bfloat16),
                pltpu.SemaphoreType.DMA((req_local,)),
                pltpu.SemaphoreType.DMA,
                pltpu.SemaphoreType.DMA((2,)),
            ],
            compiler_params=pltpu.CompilerParams(vmem_limit_bytes=6 * MIB),
            name="finish",
        )(seq_lens, *received, q_lat, q_rope)
        return c_cache, jnp.transpose(k_turned, (0, 2, 1)), o_lat

    return jax.shard_map(local_step, mesh=mesh, in_specs=(seq_spec, seq_spec, P(None), P("x", None), P("x", None), P("dp"), req_spec, req_spec), out_specs=(req_spec, req_spec, req_spec), check_vma=False)
```

```python
import functools
import math

import jax
import jax.numpy as jnp
from jax import lax
from jax.experimental import pallas as pl
from jax.experimental.pallas import tpu as pltpu
from jax.sharding import PartitionSpec as P

NORM_EPS = 1e-6
MASKED = -1e30
MESH = pl.DeviceIdType.MESH
MIB = 2**20
CORES = 2
TOGETHER = 8

STAGES = (
    ((2, 2), (0, 0)),
    ((1, 1), (-1, -1)),
    ((1, -1), (-1, 1)),
    ((1, 2), (-1, 0)),
    ((-1, 2), (1, 0)),
    ((2, 1), (0, -1)),
    ((2, -1), (0, 1)),
    ((2, 0), (0, 2)),
)
OFFSETS = tuple(offset for stage in STAGES for offset in stage)
OWN = OFFSETS.index((0, 0))
EARLY = ((0, 1), (2, 3), (4, 5), (6, 7), (9, 10), (11, 12))
LATE = ((8, 13), (14, 15))
NT = (((1,), (1,)), ((), ()))


def table(values, index):
    if isinstance(index, int):
        return values[index]
    out = jnp.int32(values[0])
    for place, value in enumerate(values[1:], 1):
        out = jnp.where(index == place, jnp.int32(value), out)
    return out


def chip_at(me, side, place, sign=1):
    chip = me // CORES
    dx = table([(sign * dx) % side for dx, _ in OFFSETS], place)
    dy = table([(sign * dy) % side for _, dy in OFFSETS], place)
    return lax.rem(chip // side + dy, side) * side + lax.rem(lax.rem(chip, side) + dx, side)


def stack_keys(pairs_rows):
    lanes = pairs_rows.shape[-1]
    low = lax.broadcasted_iota(jnp.int32, (1, 1, lanes), 2) < lanes // 2
    zero = jnp.zeros_like(pairs_rows)
    split = [jnp.where(low, pairs_rows, zero)[:, None], jnp.where(low, zero, pairs_rows)[:, None]]
    return jnp.concatenate(split, axis=1).reshape(-1, lanes)


def attend_stage(chips, lengths, queries, c_ref, k_ref, requests, seq_local, states):
    span = CORES * seq_local
    starts = [pl.multiple_of(chip * span, span) for chip in chips]
    rows = [jnp.concatenate([c_ref[r, pl.ds(start, span), :] for start in starts], axis=0) for r in requests]
    keys = [jnp.concatenate([stack_keys(k_ref[pl.ds(chip * CORES, CORES), r]) for chip in chips], axis=0) for r in requests]
    scale = (rows[0].shape[-1] + keys[0].shape[-1] // 2) ** -0.5
    scores = [lax.dot_general(q, jnp.concatenate([row, key], axis=1), NT, preferred_element_type=jnp.float32) for q, row, key in zip(queries, rows, keys)]
    lane = lax.broadcasted_iota(jnp.int32, scores[0].shape, 1)
    position = jnp.where(lane < span, starts[0] + lane, starts[1] - span + lane)
    scores = [jnp.where(position < length, score * scale, MASKED) for score, length in zip(scores, lengths)]
    tops = [jnp.maximum(state[0], jnp.max(score, axis=-1, keepdims=True)) for state, score in zip(states, scores)]
    keeps = [jnp.exp(state[0] - top) for state, top in zip(states, tops)]
    weights = [jnp.exp(score - top) for score, top in zip(scores, tops)]
    added = [jnp.dot(weight.astype(jnp.bfloat16), row, preferred_element_type=jnp.float32) for weight, row in zip(weights, rows)]
    out = []
    for (_, total, mixed), top, keep, weight, add in zip(states, tops, keeps, weights, added):
        wide_keep = jnp.concatenate([keep] * (mixed.shape[-1] // keep.shape[-1]), axis=1)
        out.append((top, total * keep + weight, mixed * wide_keep + add))
    return out


def exchange_kernel(
    side, lens_h, c_raw, k_raw, gain_h, cos_h, sin_h, q_lat_h, q_rope_h,
    c_out, k_out, top_out, total_out, mixed_out,
    lens_s, lens_v, gain, cos, sin, q_lat, q_rope, raw, send_c, k_in, k_rows, send_k,
    small_sem, raw_sem, k_sem, c_send, c_recv, k_send, k_recv,
):
    me = lax.axis_index("x")
    group = lax.axis_index("dp")
    core = lax.rem(me, CORES)
    n_dev = side * side * CORES
    n_off = len(OFFSETS)
    seq_local = c_raw.shape[1]
    req_local, heads, _ = q_lat.shape
    pair_req = CORES * req_local
    half = cos.shape[1]
    pairs = seq_local // 2
    first_pos = me * seq_local

    barrier = pltpu.get_barrier_semaphore()

    def greet(step, carry):
        pl.semaphore_signal(barrier, inc=1, device_id=(group, lax.rem(me + step, n_dev)), device_id_type=MESH)
        return carry

    lax.fori_loop(1, n_dev, greet, 0)

    def load(o, slot):
        return pltpu.make_async_copy(c_raw.at[pl.ds(chip_at(me, side, o) * pair_req, pair_req)], raw.at[slot], raw_sem.at[slot])

    def c_copy(o, dc):
        chip = chip_at(me, side, o)
        there = lax.rem(core + dc, CORES)
        return pltpu.make_async_remote_copy(
            send_c.at[o, pl.ds(there * req_local, req_local)],
            c_out.at[:, pl.ds(pl.multiple_of(first_pos, 32), seq_local), :],
            c_send.at[o, dc],
            c_recv.at[o, dc],
            device_id=(group, chip * CORES + there),
            device_id_type=MESH,
        )

    def k_copy(o, dc):
        chip = chip_at(me, side, o)
        there = lax.rem(core + dc, CORES)
        dest = chip * CORES + there
        return pltpu.make_async_remote_copy(
            send_k.at[pl.ds(dest * req_local, req_local)],
            k_out.at[me],
            k_send.at[o, dc],
            k_recv.at[o, dc],
            device_id=(group, dest),
            device_id_type=MESH,
        )

    def norm_chip(o, slot):
        first = chip_at(me, side, o) * pair_req
        scale = gain[...].astype(jnp.float32).reshape(1, gain.shape[0])

        def body(row, carry):
            length = lens_s[0, first + row]
            x = raw[slot, row].astype(jnp.float32)
            inv = lax.rsqrt(jnp.mean(x * x, axis=-1, keepdims=True) + NORM_EPS)
            valid = first_pos + lax.broadcasted_iota(jnp.int32, inv.shape, 0) < length
            send_c[o, row] = jnp.where(valid, x * inv * scale, 0.0).astype(jnp.bfloat16)
            return carry

        lax.fori_loop(0, pair_req, body, 0, unroll=4)

    small = [
        pltpu.make_async_copy(src, dst, small_sem.at[i])
        for i, (src, dst) in enumerate(((lens_h, lens_s), (gain_h, gain), (lens_h, lens_v), (cos_h, cos), (sin_h, sin), (q_lat_h, q_lat), (q_rope_h, q_rope)))
    ]
    k_load = pltpu.make_async_copy(k_raw, k_in, k_sem)
    load(0, 0).start()
    small[0].start()
    small[1].start()
    load(1, 1).start()
    k_load.start()
    for copy in small[2:]:
        copy.start()
    small[0].wait()
    small[1].wait()
    load(0, 0).wait()
    norm_chip(0, 0)
    load(2, 0).start()
    pl.semaphore_wait(barrier, n_dev - 1)
    c_copy(0, 0).start()
    c_copy(0, 1).start()

    for copy in small[2:]:
        copy.wait()
    k_load.wait()
    cos_t = cos[...].T
    sin_t = sin[...].T
    for pair in range(pairs):
        pieces = []
        for pos in (pair, pair + pairs):
            lo = k_in[pos, :half, :].astype(jnp.float32)
            hi = k_in[pos, half:, :].astype(jnp.float32)
            c = cos_t[:, pos : pos + 1]
            s = sin_t[:, pos : pos + 1]
            keep = first_pos + pos < lens_v[...]
            pieces.append(jnp.where(keep, lo * c - hi * s, 0.0))
            pieces.append(jnp.where(keep, hi * c + lo * s, 0.0))
        k_rows[pl.ds(pair, k_rows.shape[0] // pairs, stride=pairs), :] = jnp.concatenate(pieces, axis=0).T

    def pack(step, carry):
        rows = k_rows[pl.ds(pl.multiple_of(step * req_local * pairs, 256), req_local * pairs), :].astype(jnp.bfloat16)
        send_k[pl.ds(step * req_local, req_local)] = rows.reshape(req_local, pairs, k_rows.shape[1])
        return carry

    lax.fori_loop(0, n_dev, pack, 0)

    def start_k(o):
        @pl.when(o != OWN)
        def _():
            k_copy(o, 0).start()

        k_copy(o, 1).start()

    start_k(jnp.int32(0))
    k_out[me] = send_k[pl.ds(me * req_local, req_local)]

    def produce(o, carry):
        slot = lax.rem(o, 2)
        load(o, slot).wait()
        norm_chip(o, slot)

        @pl.when(o + 2 < n_off)
        def _():
            load(o + 2, slot).start()

        @pl.when(o != OWN)
        def _():
            c_copy(o, 0).start()

        c_copy(o, 1).start()

        start_k(o)
        return carry

    lax.fori_loop(1, n_off, produce, 0)
    c_out[:, pl.ds(pl.multiple_of(first_pos, 32), seq_local), :] = send_c[OWN, pl.ds(core * req_local, req_local)]

    def clear(r, carry):
        top_out[r] = jnp.full(top_out.shape[1:], MASKED, jnp.float32)
        total_out[r] = jnp.zeros(total_out.shape[1:], jnp.float32)
        mixed_out[r] = jnp.zeros(mixed_out.shape[1:], jnp.float32)
        return carry

    lax.fori_loop(0, req_local, clear, 0)

    def arrived(o):
        @pl.when(o != OWN)
        def _():
            c_copy(o, 0).wait_recv()
            k_copy(o, 0).wait_recv()

        c_copy(o, 1).wait_recv()
        k_copy(o, 1).wait_recv()

    def attend(stage, carry):
        places = [table([pair[i] for pair in EARLY], stage) for i in range(2)]
        chips = [chip_at(me, side, place, -1) for place in places]
        for place in places:
            arrived(place)

        def some(step, carry):
            requests = [step * TOGETHER + i for i in range(TOGETHER)]
            queries = [jnp.concatenate([q_lat[r], q_rope[r], q_rope[r]], axis=1) for r in requests]
            lengths = [lens_s[0, me * req_local + r] for r in requests]
            states = [(top_out[r], total_out[r], mixed_out[r]) for r in requests]
            states = attend_stage(chips, lengths, queries, c_out, k_out, requests, seq_local, states)
            for r, state in zip(requests, states):
                top_out[r], total_out[r], mixed_out[r] = state
            return carry

        lax.fori_loop(0, req_local // TOGETHER, some, 0)
        return carry

    lax.fori_loop(0, len(EARLY), attend, 0)
    for pair in LATE:
        for place in pair:
            arrived(jnp.int32(place))

    def sent(o, carry):
        for copy in (c_copy, k_copy):

            @pl.when(o != OWN)
            def _():
                copy(o, 0).wait_send()

            copy(o, 1).wait_send()
        return carry

    lax.fori_loop(0, n_off, sent, 0)


def finish_kernel(side, lens_h, c_in, k_in, top, total, mixed, q_lat_h, q_rope_h, c_cache, k_cache, o_lat, lens_s, turned, q_lat, q_rope, o_here, c_sem, k_sem, o_sem, small_sem):
    me = lax.axis_index("x")
    n_req, seq, _ = c_in.shape
    seq_local = seq // (side * side * CORES)

    def c_copy(r):
        return pltpu.make_async_copy(c_in.at[r], c_cache.at[r], c_sem.at[r])

    def start(r, carry):
        c_copy(r).start()
        return carry

    small = [pltpu.make_async_copy(src, dst, small_sem.at[i]) for i, (src, dst) in enumerate(((lens_h, lens_s), (q_lat_h, q_lat), (q_rope_h, q_rope)))]
    for copy in small:
        copy.start()
    lax.fori_loop(0, n_req, start, 0)

    k_copy = pltpu.make_async_copy(turned, k_cache, k_sem)
    rope = turned.shape[1]
    shape = (rope, 2 * rope)
    eye = (lax.broadcasted_iota(jnp.int32, shape, 0) == lax.rem(lax.broadcasted_iota(jnp.int32, shape, 1), rope)).astype(jnp.bfloat16)

    def turn(step, carry):
        requests = [step * 4 + i for i in range(4)]
        results = [lax.dot_general(eye, stack_keys(k_in[:, r]), NT, preferred_element_type=jnp.float32) for r in requests]
        for r, result in zip(requests, results):
            turned[r] = result.astype(jnp.bfloat16)
        return carry

    lax.fori_loop(0, n_req // 4, turn, 0)
    k_copy.start()
    for copy in small:
        copy.wait()

    def some(step, carry):
        requests = [step * TOGETHER + i for i in range(TOGETHER)]
        queries = [jnp.concatenate([q_lat[r], q_rope[r], q_rope[r]], axis=1) for r in requests]
        lengths = [lens_s[0, me * n_req + r] for r in requests]
        states = [(top[r], total[r], mixed[r]) for r in requests]
        for pair in LATE:
            chips = [chip_at(me, side, place, -1) for place in pair]
            states = attend_stage(chips, lengths, queries, c_in, k_in, requests, seq_local, states)
        for r, (_, weights, values) in zip(requests, states):
            o_here[r] = (values / jnp.sum(weights, axis=-1, keepdims=True)).astype(jnp.bfloat16)
        return carry

    lax.fori_loop(0, n_req // TOGETHER, some, 0)
    o_copy = pltpu.make_async_copy(o_here, o_lat, o_sem)
    o_copy.start()

    def finish(r, carry):
        c_copy(r).wait()
        return carry

    lax.fori_loop(0, n_req, finish, 0)
    k_copy.wait()
    o_copy.wait()


def solution(mesh):
    seq_spec = P("dp", "x", None)
    req_spec = P(("dp", "x"), None, None)
    vmem = pl.BlockSpec(memory_space=pltpu.VMEM)
    anywhere = pl.BlockSpec(memory_space=pl.ANY)
    n_dev = mesh.shape["x"]
    side = math.isqrt(n_dev // CORES)

    def local_step(c_raw, k_raw, norm_gain, rope_cos, rope_sin, seq_lens, q_lat, q_rope):
        n_all, seq_local, width = c_raw.shape
        rope = k_raw.shape[-1]
        req_local, heads, _ = q_lat.shape
        seq = n_dev * seq_local
        pairs = seq_local // 2
        n_off = len(OFFSETS)
        lanes = 2 * CORES * seq_local
        lens_row = seq_lens.reshape(1, n_all)
        state = pltpu.VMEM((req_local, heads, lanes), jnp.float32)
        received = pl.pallas_call(
            functools.partial(exchange_kernel, side),
            out_shape=(
                pltpu.VMEM((req_local, seq, width), jnp.bfloat16),
                pltpu.VMEM((n_dev, req_local, pairs, 2 * rope), jnp.bfloat16),
                state,
                state,
                pltpu.VMEM((req_local, heads, width), jnp.float32),
            ),
            in_specs=[anywhere] * 8,
            out_specs=(vmem,) * 5,
            scratch_shapes=[
                pltpu.SMEM((1, n_all), jnp.int32),
                pltpu.VMEM((1, n_all), jnp.int32),
                pltpu.VMEM((width,), jnp.bfloat16),
                pltpu.VMEM(rope_cos.shape, jnp.float32),
                pltpu.VMEM(rope_sin.shape, jnp.float32),
                pltpu.VMEM(q_lat.shape, jnp.bfloat16),
                pltpu.VMEM(q_rope.shape, jnp.bfloat16),
                pltpu.VMEM((2, CORES * req_local, seq_local, width), jnp.bfloat16),
                pltpu.VMEM((n_off, CORES * req_local, seq_local, width), jnp.bfloat16),
                pltpu.VMEM((seq_local, rope, n_all), jnp.bfloat16),
                pltpu.VMEM((n_all * pairs, 2 * rope), jnp.float32),
                pltpu.VMEM((n_all, pairs, 2 * rope), jnp.bfloat16),
                pltpu.SemaphoreType.DMA((7,)),
                pltpu.SemaphoreType.DMA((2,)),
                pltpu.SemaphoreType.DMA,
                pltpu.SemaphoreType.DMA((n_off, CORES)),
                pltpu.SemaphoreType.DMA((n_off, CORES)),
                pltpu.SemaphoreType.DMA((n_off, CORES)),
                pltpu.SemaphoreType.DMA((n_off, CORES)),
            ],
            compiler_params=pltpu.CompilerParams(collective_id=0, has_side_effects=True, vmem_limit_bytes=42 * MIB),
            name="exchange",
        )(lens_row, c_raw, jnp.transpose(k_raw, (1, 2, 0)), norm_gain, rope_cos, rope_sin, q_lat, q_rope)
        c_cache, k_turned, o_lat = pl.pallas_call(
            functools.partial(finish_kernel, side),
            out_shape=(
                jax.ShapeDtypeStruct((req_local, seq, width), jnp.bfloat16),
                jax.ShapeDtypeStruct((req_local, rope, seq), jnp.bfloat16),
                jax.ShapeDtypeStruct((req_local, heads, width), jnp.bfloat16),
            ),
            in_specs=[anywhere] + [vmem] * 5 + [anywhere] * 2,
            out_specs=(anywhere, anywhere, anywhere),
            scratch_shapes=[
                pltpu.SMEM((1, n_all), jnp.int32),
                pltpu.VMEM((req_local, rope, seq), jnp.bfloat16),
                pltpu.VMEM(q_lat.shape, jnp.bfloat16),
                pltpu.VMEM(q_rope.shape, jnp.bfloat16),
                pltpu.VMEM(q_lat.shape, jnp.bfloat16),
                pltpu.SemaphoreType.DMA((req_local,)),
                pltpu.SemaphoreType.DMA,
                pltpu.SemaphoreType.DMA,
                pltpu.SemaphoreType.DMA((3,)),
            ],
            compiler_params=pltpu.CompilerParams(vmem_limit_bytes=6 * MIB),
            name="finish",
        )(lens_row, *received, q_lat, q_rope)
        return c_cache, jnp.transpose(k_turned, (0, 2, 1)), o_lat

    return jax.shard_map(local_step, mesh=mesh, in_specs=(seq_spec, seq_spec, P(None), P("x", None), P("x", None), P("dp"), req_spec, req_spec), out_specs=(req_spec, req_spec, req_spec), check_vma=False)
```

```python
import functools
import math

import jax
import jax.numpy as jnp
from jax import lax
from jax.experimental import pallas as pl
from jax.experimental.pallas import tpu as pltpu
from jax.sharding import PartitionSpec as P

NORM_EPS = 1e-6
MASKED = -1e30
MESH = pl.DeviceIdType.MESH
MIB = 2**20
CORES = 2
TOGETHER = 8

STAGES = (
    ((2, 2), (0, 0)),
    ((2, -1), (0, 1)),
    ((2, 1), (0, -1)),
    ((2, 0), (0, 2)),
    ((1, 2), (-1, 0)),
    ((-1, 2), (1, 0)),
    ((1, 1), (-1, -1)),
    ((1, -1), (-1, 1)),
)
OFFSETS = tuple(offset for stage in STAGES for offset in stage)
OWN = OFFSETS.index((0, 0))
EARLY = ((0, 1), (2, 3), (4, 5), (6, 7), (8, 9), (10, 11))
LATE = ((12, 13), (14, 15))
NT = (((1,), (1,)), ((), ()))


def table(values, index):
    if isinstance(index, int):
        return values[index]
    out = jnp.int32(values[0])
    for place, value in enumerate(values[1:], 1):
        out = jnp.where(index == place, jnp.int32(value), out)
    return out


def chip_at(me, side, place, sign=1):
    chip = me // CORES
    dx = table([(sign * dx) % side for dx, _ in OFFSETS], place)
    dy = table([(sign * dy) % side for _, dy in OFFSETS], place)
    return lax.rem(chip // side + dy, side) * side + lax.rem(lax.rem(chip, side) + dx, side)


def stack_keys(pairs_rows):
    lanes = pairs_rows.shape[-1]
    low = lax.broadcasted_iota(jnp.int32, (1, 1, lanes), 2) < lanes // 2
    zero = jnp.zeros_like(pairs_rows)
    split = [jnp.where(low, pairs_rows, zero)[:, None], jnp.where(low, zero, pairs_rows)[:, None]]
    return jnp.concatenate(split, axis=1).reshape(-1, lanes)


def attend_stage(chips, lengths, queries, c_ref, k_ref, requests, seq_local, states):
    span = CORES * seq_local
    starts = [pl.multiple_of(chip * span, span) for chip in chips]
    rows = [jnp.concatenate([c_ref[r, pl.ds(start, span), :] for start in starts], axis=0) for r in requests]
    keys = [jnp.concatenate([stack_keys(k_ref[pl.ds(chip * CORES, CORES), r]) for chip in chips], axis=0) for r in requests]
    scale = (rows[0].shape[-1] + keys[0].shape[-1] // 2) ** -0.5
    scores = [lax.dot_general(q, jnp.concatenate([row, key], axis=1), NT, preferred_element_type=jnp.float32) for q, row, key in zip(queries, rows, keys)]
    lane = lax.broadcasted_iota(jnp.int32, scores[0].shape, 1)
    position = jnp.where(lane < span, starts[0] + lane, starts[1] - span + lane)
    scores = [jnp.where(position < length, score * scale, MASKED) for score, length in zip(scores, lengths)]
    tops = [jnp.maximum(state[0], jnp.max(score, axis=-1, keepdims=True)) for state, score in zip(states, scores)]
    keeps = [jnp.exp(state[0] - top) for state, top in zip(states, tops)]
    weights = [jnp.exp(score - top) for score, top in zip(scores, tops)]
    added = [jnp.dot(weight.astype(jnp.bfloat16), row, preferred_element_type=jnp.float32) for weight, row in zip(weights, rows)]
    out = []
    for (_, total, mixed), top, keep, weight, add in zip(states, tops, keeps, weights, added):
        wide_keep = jnp.concatenate([keep] * (mixed.shape[-1] // keep.shape[-1]), axis=1)
        out.append((top, total * keep + weight, mixed * wide_keep + add))
    return out


def exchange_kernel(
    side, lens_h, c_raw, k_raw, gain_h, cos_h, sin_h, q_lat_h, q_rope_h,
    c_out, k_out, top_out, total_out, mixed_out, lens_v, q_lat, q_rope,
    lens_s, gain, cos, sin, raw, send_c, k_in, k_rows, send_k,
    small_sem, half_sem, raw_sem, k_sem, c_send, c_recv, k_send, k_recv,
):
    me = lax.axis_index("x")
    group = lax.axis_index("dp")
    core = lax.rem(me, CORES)
    n_dev = side * side * CORES
    n_off = len(OFFSETS)
    seq_local = c_raw.shape[1]
    req_local, heads, _ = q_lat.shape
    pair_req = CORES * req_local
    half = cos.shape[1]
    pairs = seq_local // 2
    first_pos = me * seq_local

    barrier = pltpu.get_barrier_semaphore()

    def greet(step, carry):
        pl.semaphore_signal(barrier, inc=1, device_id=(group, lax.rem(me + step, n_dev)), device_id_type=MESH)
        return carry

    def load(o, slot):
        return pltpu.make_async_copy(c_raw.at[pl.ds(chip_at(me, side, o) * pair_req, pair_req)], raw.at[slot], raw_sem.at[slot])

    def load_half(dc):
        there = lax.rem(core + dc, CORES) * req_local
        return pltpu.make_async_copy(c_raw.at[pl.ds(chip_at(me, side, 0) * pair_req + there, req_local)], raw.at[0, pl.ds(there, req_local)], half_sem.at[dc])

    def c_copy(o, dc):
        chip = chip_at(me, side, o)
        there = lax.rem(core + dc, CORES)
        return pltpu.make_async_remote_copy(
            send_c.at[o, pl.ds(there * req_local, req_local)],
            c_out.at[:, pl.ds(pl.multiple_of(first_pos, 32), seq_local), :],
            c_send.at[o, dc],
            c_recv.at[o, dc],
            device_id=(group, chip * CORES + there),
            device_id_type=MESH,
        )

    def k_copy(o, dc):
        chip = chip_at(me, side, o)
        there = lax.rem(core + dc, CORES)
        dest = chip * CORES + there
        return pltpu.make_async_remote_copy(
            send_k.at[pl.ds(dest * req_local, req_local)],
            k_out.at[me],
            k_send.at[o, dc],
            k_recv.at[o, dc],
            device_id=(group, dest),
            device_id_type=MESH,
        )

    def norm_rows(o, slot, start, count):
        first = chip_at(me, side, o) * pair_req
        scale = gain[...].astype(jnp.float32).reshape(1, gain.shape[0])

        def body(step, carry):
            row = start + step
            length = lens_s[0, first + row]
            x = raw[slot, row].astype(jnp.float32)
            inv = lax.rsqrt(jnp.mean(x * x, axis=-1, keepdims=True) + NORM_EPS)
            valid = first_pos + lax.broadcasted_iota(jnp.int32, inv.shape, 0) < length
            send_c[o, row] = jnp.where(valid, x * inv * scale, 0.0).astype(jnp.bfloat16)
            return carry

        lax.fori_loop(0, count, body, 0, unroll=4)

    small = [
        pltpu.make_async_copy(src, dst, small_sem.at[i])
        for i, (src, dst) in enumerate(((lens_h, lens_s), (gain_h, gain), (lens_h, lens_v), (cos_h, cos), (sin_h, sin), (q_lat_h, q_lat), (q_rope_h, q_rope)))
    ]
    k_load = pltpu.make_async_copy(k_raw, k_in, k_sem)
    load_half(0).start()
    small[0].start()
    small[1].start()
    lax.fori_loop(1, n_dev, greet, 0)
    load_half(1).start()
    load(1, 1).start()
    k_load.start()
    for copy in small[2:]:
        copy.start()
    small[0].wait()
    small[1].wait()
    load_half(0).wait()
    norm_rows(0, 0, core * req_local, req_local)
    pl.semaphore_wait(barrier, n_dev - 1)
    c_copy(0, 0).start()
    load_half(1).wait()
    norm_rows(0, 0, (CORES - 1 - core) * req_local, req_local)
    c_copy(0, 1).start()
    load(2, 0).start()

    for copy in small[2:]:
        copy.wait()
    k_load.wait()
    cos_t = cos[...].T
    sin_t = sin[...].T
    for pair in range(pairs):
        pieces = []
        for pos in (pair, pair + pairs):
            lo = k_in[pos, :half, :].astype(jnp.float32)
            hi = k_in[pos, half:, :].astype(jnp.float32)
            c = cos_t[:, pos : pos + 1]
            s = sin_t[:, pos : pos + 1]
            keep = first_pos + pos < lens_v[...]
            pieces.append(jnp.where(keep, lo * c - hi * s, 0.0))
            pieces.append(jnp.where(keep, hi * c + lo * s, 0.0))
        k_rows[pl.ds(pair, k_rows.shape[0] // pairs, stride=pairs), :] = jnp.concatenate(pieces, axis=0).T

    def pack(step, carry):
        rows = k_rows[pl.ds(pl.multiple_of(step * req_local * pairs, 256), req_local * pairs), :].astype(jnp.bfloat16)
        send_k[pl.ds(step * req_local, req_local)] = rows.reshape(req_local, pairs, k_rows.shape[1])
        return carry

    lax.fori_loop(0, n_dev, pack, 0)

    def start_k(o):
        @pl.when(o != OWN)
        def _():
            k_copy(o, 0).start()

        k_copy(o, 1).start()

    start_k(jnp.int32(0))
    k_out[me] = send_k[pl.ds(me * req_local, req_local)]

    def produce(o, carry):
        slot = lax.rem(o, 2)
        load(o, slot).wait()
        norm_rows(o, slot, 0, pair_req)

        @pl.when(o + 2 < n_off)
        def _():
            load(o + 2, slot).start()

        @pl.when(o != OWN)
        def _():
            c_copy(o, 0).start()

        c_copy(o, 1).start()

        start_k(o)
        return carry

    lax.fori_loop(1, n_off, produce, 0)
    c_out[:, pl.ds(pl.multiple_of(first_pos, 32), seq_local), :] = send_c[OWN, pl.ds(core * req_local, req_local)]

    def clear(r, carry):
        top_out[r] = jnp.full(top_out.shape[1:], MASKED, jnp.float32)
        total_out[r] = jnp.zeros(total_out.shape[1:], jnp.float32)
        mixed_out[r] = jnp.zeros(mixed_out.shape[1:], jnp.float32)
        return carry

    lax.fori_loop(0, req_local, clear, 0)

    def arrived(o):
        @pl.when(o != OWN)
        def _():
            c_copy(o, 0).wait_recv()
            k_copy(o, 0).wait_recv()

        c_copy(o, 1).wait_recv()
        k_copy(o, 1).wait_recv()

    def attend(stage, carry):
        places = [table([pair[i] for pair in EARLY], stage) for i in range(2)]
        chips = [chip_at(me, side, place, -1) for place in places]
        for place in places:
            arrived(place)

        def some(step, carry):
            requests = [step * TOGETHER + i for i in range(TOGETHER)]
            queries = [jnp.concatenate([q_lat[r], q_rope[r], q_rope[r]], axis=1) for r in requests]
            lengths = [lens_s[0, me * req_local + r] for r in requests]
            states = [(top_out[r], total_out[r], mixed_out[r]) for r in requests]
            states = attend_stage(chips, lengths, queries, c_out, k_out, requests, seq_local, states)
            for r, state in zip(requests, states):
                top_out[r], total_out[r], mixed_out[r] = state
            return carry

        lax.fori_loop(0, req_local // TOGETHER, some, 0)
        return carry

    lax.fori_loop(0, len(EARLY), attend, 0)
    for pair in LATE:
        for place in pair:
            arrived(jnp.int32(place))

    def sent(o, carry):
        for copy in (c_copy, k_copy):

            @pl.when(o != OWN)
            def _():
                copy(o, 0).wait_send()

            copy(o, 1).wait_send()
        return carry

    lax.fori_loop(0, n_off, sent, 0)


def finish_kernel(side, c_in, k_in, top, total, mixed, lens_v, q_lat, q_rope, c_cache, k_cache, o_lat, lens_s, turned, o_here, c_sem, k_sem, o_sem, lens_sem):
    me = lax.axis_index("x")
    n_req, seq, _ = c_in.shape
    seq_local = seq // (side * side * CORES)

    def c_copy(r):
        return pltpu.make_async_copy(c_in.at[r], c_cache.at[r], c_sem.at[r])

    def start(r, carry):
        c_copy(r).start()
        return carry

    lens_copy = pltpu.make_async_copy(lens_v, lens_s, lens_sem)
    lens_copy.start()
    lax.fori_loop(0, n_req, start, 0)

    k_copy = pltpu.make_async_copy(turned, k_cache, k_sem)
    rope = turned.shape[1]
    shape = (rope, 2 * rope)
    eye = (lax.broadcasted_iota(jnp.int32, shape, 0) == lax.rem(lax.broadcasted_iota(jnp.int32, shape, 1), rope)).astype(jnp.bfloat16)

    def turn(step, carry):
        requests = [step * 4 + i for i in range(4)]
        results = [lax.dot_general(eye, stack_keys(k_in[:, r]), NT, preferred_element_type=jnp.float32) for r in requests]
        for r, result in zip(requests, results):
            turned[r] = result.astype(jnp.bfloat16)
        return carry

    lax.fori_loop(0, n_req // 4, turn, 0)
    k_copy.start()
    lens_copy.wait()

    def some(step, carry):
        requests = [step * TOGETHER + i for i in range(TOGETHER)]
        queries = [jnp.concatenate([q_lat[r], q_rope[r], q_rope[r]], axis=1) for r in requests]
        lengths = [lens_s[0, me * n_req + r] for r in requests]
        states = [(top[r], total[r], mixed[r]) for r in requests]
        for pair in LATE:
            chips = [chip_at(me, side, place, -1) for place in pair]
            states = attend_stage(chips, lengths, queries, c_in, k_in, requests, seq_local, states)
        for r, (_, weights, values) in zip(requests, states):
            o_here[r] = (values / jnp.sum(weights, axis=-1, keepdims=True)).astype(jnp.bfloat16)
        return carry

    lax.fori_loop(0, n_req // TOGETHER, some, 0)
    o_copy = pltpu.make_async_copy(o_here, o_lat, o_sem)
    o_copy.start()

    def finish(r, carry):
        c_copy(r).wait()
        return carry

    lax.fori_loop(0, n_req, finish, 0)
    k_copy.wait()
    o_copy.wait()


def solution(mesh):
    seq_spec = P("dp", "x", None)
    req_spec = P(("dp", "x"), None, None)
    vmem = pl.BlockSpec(memory_space=pltpu.VMEM)
    anywhere = pl.BlockSpec(memory_space=pl.ANY)
    n_dev = mesh.shape["x"]
    side = math.isqrt(n_dev // CORES)

    def local_step(c_raw, k_raw, norm_gain, rope_cos, rope_sin, seq_lens, q_lat, q_rope):
        n_all, seq_local, width = c_raw.shape
        rope = k_raw.shape[-1]
        req_local, heads, _ = q_lat.shape
        seq = n_dev * seq_local
        pairs = seq_local // 2
        n_off = len(OFFSETS)
        lanes = 2 * CORES * seq_local
        lens_row = seq_lens.reshape(1, n_all)
        state = pltpu.VMEM((req_local, heads, lanes), jnp.float32)
        received = pl.pallas_call(
            functools.partial(exchange_kernel, side),
            out_shape=(
                pltpu.VMEM((req_local, seq, width), jnp.bfloat16),
                pltpu.VMEM((n_dev, req_local, pairs, 2 * rope), jnp.bfloat16),
                state,
                state,
                pltpu.VMEM((req_local, heads, width), jnp.float32),
                pltpu.VMEM((1, n_all), jnp.int32),
                pltpu.VMEM(q_lat.shape, jnp.bfloat16),
                pltpu.VMEM(q_rope.shape, jnp.bfloat16),
            ),
            in_specs=[anywhere] * 8,
            out_specs=(vmem,) * 8,
            scratch_shapes=[
                pltpu.SMEM((1, n_all), jnp.int32),
                pltpu.VMEM((width,), jnp.bfloat16),
                pltpu.VMEM(rope_cos.shape, jnp.float32),
                pltpu.VMEM(rope_sin.shape, jnp.float32),
                pltpu.VMEM((2, CORES * req_local, seq_local, width), jnp.bfloat16),
                pltpu.VMEM((n_off, CORES * req_local, seq_local, width), jnp.bfloat16),
                pltpu.VMEM((seq_local, rope, n_all), jnp.bfloat16),
                pltpu.VMEM((n_all * pairs, 2 * rope), jnp.float32),
                pltpu.VMEM((n_all, pairs, 2 * rope), jnp.bfloat16),
                pltpu.SemaphoreType.DMA((7,)),
                pltpu.SemaphoreType.DMA((CORES,)),
                pltpu.SemaphoreType.DMA((2,)),
                pltpu.SemaphoreType.DMA,
                pltpu.SemaphoreType.DMA((n_off, CORES)),
                pltpu.SemaphoreType.DMA((n_off, CORES)),
                pltpu.SemaphoreType.DMA((n_off, CORES)),
                pltpu.SemaphoreType.DMA((n_off, CORES)),
            ],
            compiler_params=pltpu.CompilerParams(collective_id=0, has_side_effects=True, vmem_limit_bytes=42 * MIB),
            name="exchange",
        )(lens_row, c_raw, jnp.transpose(k_raw, (1, 2, 0)), norm_gain, rope_cos, rope_sin, q_lat, q_rope)
        c_cache, k_turned, o_lat = pl.pallas_call(
            functools.partial(finish_kernel, side),
            out_shape=(
                jax.ShapeDtypeStruct((req_local, seq, width), jnp.bfloat16),
                jax.ShapeDtypeStruct((req_local, rope, seq), jnp.bfloat16),
                jax.ShapeDtypeStruct((req_local, heads, width), jnp.bfloat16),
            ),
            in_specs=[vmem] * 8,
            out_specs=(anywhere, anywhere, anywhere),
            scratch_shapes=[
                pltpu.SMEM((1, n_all), jnp.int32),
                pltpu.VMEM((req_local, rope, seq), jnp.bfloat16),
                pltpu.VMEM(q_lat.shape, jnp.bfloat16),
                pltpu.SemaphoreType.DMA((req_local,)),
                pltpu.SemaphoreType.DMA,
                pltpu.SemaphoreType.DMA,
                pltpu.SemaphoreType.DMA,
            ],
            compiler_params=pltpu.CompilerParams(vmem_limit_bytes=6 * MIB),
            name="finish",
        )(*received)
        return c_cache, jnp.transpose(k_turned, (0, 2, 1)), o_lat

    return jax.shard_map(local_step, mesh=mesh, in_specs=(seq_spec, seq_spec, P(None), P("x", None), P("x", None), P("dp"), req_spec, req_spec), out_specs=(req_spec, req_spec, req_spec), check_vma=False)
```

```python
import functools
import math

import jax
import jax.numpy as jnp
from jax import lax
from jax.experimental import pallas as pl
from jax.experimental.pallas import tpu as pltpu
from jax.sharding import PartitionSpec as P

NORM_EPS = 1e-6
MASKED = -1e30
MESH = pl.DeviceIdType.MESH
MIB = 2**20
CORES = 2
TOGETHER = 8

STAGES = (
    ((2, 2), (0, 0)),
    ((2, -1), (0, 1)),
    ((2, 1), (0, -1)),
    ((2, 0), (0, 2)),
    ((1, 2), (-1, 0)),
    ((-1, 2), (1, 0)),
    ((1, 1), (-1, -1)),
    ((1, -1), (-1, 1)),
)
OFFSETS = tuple(offset for stage in STAGES for offset in stage)
OWN = OFFSETS.index((0, 0))
EARLY = ((0, 1), (2, 3), (4, 5), (6, 7), (8, 9), (10, 11))
LATE = ((12, 13), (14, 15))
NT = (((1,), (1,)), ((), ()))


def table(values, index):
    if isinstance(index, int):
        return values[index]
    out = jnp.int32(values[0])
    for place, value in enumerate(values[1:], 1):
        out = jnp.where(index == place, jnp.int32(value), out)
    return out


def chip_at(me, side, place, sign=1):
    chip = me // CORES
    dx = table([(sign * dx) % side for dx, _ in OFFSETS], place)
    dy = table([(sign * dy) % side for _, dy in OFFSETS], place)
    return lax.rem(chip // side + dy, side) * side + lax.rem(lax.rem(chip, side) + dx, side)


def stack_keys(pairs_rows):
    lanes = pairs_rows.shape[-1]
    low = lax.broadcasted_iota(jnp.int32, (1, 1, lanes), 2) < lanes // 2
    zero = jnp.zeros_like(pairs_rows)
    split = [jnp.where(low, pairs_rows, zero)[:, None], jnp.where(low, zero, pairs_rows)[:, None]]
    return jnp.concatenate(split, axis=1).reshape(-1, lanes)


def attend_stage(chips, lengths, queries, c_ref, k_ref, requests, seq_local, states):
    span = CORES * seq_local
    starts = [pl.multiple_of(chip * span, span) for chip in chips]
    rows = [jnp.concatenate([c_ref[r, pl.ds(start, span), :] for start in starts], axis=0) for r in requests]
    keys = [jnp.concatenate([stack_keys(k_ref[pl.ds(chip * CORES, CORES), r]) for chip in chips], axis=0) for r in requests]
    scale = (rows[0].shape[-1] + keys[0].shape[-1] // 2) ** -0.5
    scores = [lax.dot_general(q, jnp.concatenate([row, key], axis=1), NT, preferred_element_type=jnp.float32) for q, row, key in zip(queries, rows, keys)]
    lane = lax.broadcasted_iota(jnp.int32, scores[0].shape, 1)
    position = jnp.where(lane < span, starts[0] + lane, starts[1] - span + lane)
    scores = [jnp.where(position < length, score * scale, MASKED) for score, length in zip(scores, lengths)]
    tops = [jnp.maximum(state[0], jnp.max(score, axis=-1, keepdims=True)) for state, score in zip(states, scores)]
    keeps = [jnp.exp(state[0] - top) for state, top in zip(states, tops)]
    weights = [jnp.exp(score - top) for score, top in zip(scores, tops)]
    added = [jnp.dot(weight.astype(jnp.bfloat16), row, preferred_element_type=jnp.float32) for weight, row in zip(weights, rows)]
    out = []
    for (_, total, mixed), top, keep, weight, add in zip(states, tops, keeps, weights, added):
        wide_keep = jnp.concatenate([keep] * (mixed.shape[-1] // keep.shape[-1]), axis=1)
        out.append((top, total * keep + weight, mixed * wide_keep + add))
    return out


def exchange_kernel(
    side, lens_h, c_raw, k_raw, gain_h, cos_h, sin_h, q_lat_h, q_rope_h,
    c_out, k_out, top_out, total_out, mixed_out, lens_v, q_lat, q_rope,
    lens_s, gain, cos, sin, raw, send_c, k_in, k_rows, send_k,
    small_sem, half_sem, raw_sem, k_sem, c_send, c_recv, k_send, k_recv,
):
    me = lax.axis_index("x")
    group = lax.axis_index("dp")
    core = lax.rem(me, CORES)
    n_dev = side * side * CORES
    n_off = len(OFFSETS)
    seq_local = c_raw.shape[1]
    req_local, heads, _ = q_lat.shape
    pair_req = CORES * req_local
    half = cos.shape[1]
    pairs = seq_local // 2
    first_pos = me * seq_local

    barrier = pltpu.get_barrier_semaphore()

    def greet(step, carry):
        pl.semaphore_signal(barrier, inc=1, device_id=(group, lax.rem(me + step, n_dev)), device_id_type=MESH)
        return carry

    def load(o, slot):
        return pltpu.make_async_copy(c_raw.at[pl.ds(chip_at(me, side, o) * pair_req, pair_req)], raw.at[slot], raw_sem.at[slot])

    def load_half(dc):
        there = lax.rem(core + dc, CORES) * req_local
        return pltpu.make_async_copy(c_raw.at[pl.ds(chip_at(me, side, 0) * pair_req + there, req_local)], raw.at[0, pl.ds(there, req_local)], half_sem.at[dc])

    def c_copy(o, dc):
        chip = chip_at(me, side, o)
        there = lax.rem(core + dc, CORES)
        return pltpu.make_async_remote_copy(
            send_c.at[o, pl.ds(there * req_local, req_local)],
            c_out.at[:, pl.ds(pl.multiple_of(first_pos, 32), seq_local), :],
            c_send.at[o, dc],
            c_recv.at[o, dc],
            device_id=(group, chip * CORES + there),
            device_id_type=MESH,
        )

    def k_copy(o, dc):
        chip = chip_at(me, side, o)
        there = lax.rem(core + dc, CORES)
        dest = chip * CORES + there
        return pltpu.make_async_remote_copy(
            send_k.at[pl.ds(dest * req_local, req_local)],
            k_out.at[me],
            k_send.at[o, dc],
            k_recv.at[o, dc],
            device_id=(group, dest),
            device_id_type=MESH,
        )

    def norm_rows(o, slot, start, count):
        first = chip_at(me, side, o) * pair_req
        scale = gain[...].astype(jnp.float32).reshape(1, gain.shape[0])

        def body(step, carry):
            row = start + step
            length = lens_s[0, first + row]
            x = raw[slot, row].astype(jnp.float32)
            inv = lax.rsqrt(jnp.mean(x * x, axis=-1, keepdims=True) + NORM_EPS)
            valid = first_pos + lax.broadcasted_iota(jnp.int32, inv.shape, 0) < length
            send_c[o, row] = jnp.where(valid, x * inv * scale, 0.0).astype(jnp.bfloat16)
            return carry

        lax.fori_loop(0, count, body, 0, unroll=4)

    small = [
        pltpu.make_async_copy(src, dst, small_sem.at[i])
        for i, (src, dst) in enumerate(((lens_h, lens_s), (gain_h, gain), (lens_h, lens_v), (cos_h, cos), (sin_h, sin), (q_lat_h, q_lat), (q_rope_h, q_rope)))
    ]
    k_load = pltpu.make_async_copy(k_raw, k_in, k_sem)
    load_half(0).start()
    small[0].start()
    small[1].start()
    lax.fori_loop(1, n_dev, greet, 0)
    load_half(1).start()
    load(1, 1).start()
    k_load.start()
    for copy in small[2:]:
        copy.start()
    small[0].wait()
    small[1].wait()
    load_half(0).wait()
    norm_rows(0, 0, core * req_local, req_local)
    pl.semaphore_wait(barrier, n_dev - 1)
    c_copy(0, 0).start()
    load_half(1).wait()
    norm_rows(0, 0, (CORES - 1 - core) * req_local, req_local)
    c_copy(0, 1).start()
    load(2, 0).start()

    for copy in small[2:]:
        copy.wait()
    k_load.wait()
    cos_t = cos[...].T
    sin_t = sin[...].T
    for pair in range(pairs):
        pieces = []
        for pos in (pair, pair + pairs):
            lo = k_in[pos, :half, :].astype(jnp.float32)
            hi = k_in[pos, half:, :].astype(jnp.float32)
            c = cos_t[:, pos : pos + 1]
            s = sin_t[:, pos : pos + 1]
            keep = first_pos + pos < lens_v[...]
            pieces.append(jnp.where(keep, lo * c - hi * s, 0.0))
            pieces.append(jnp.where(keep, hi * c + lo * s, 0.0))
        k_rows[pl.ds(pair, k_rows.shape[0] // pairs, stride=pairs), :] = jnp.concatenate(pieces, axis=0).T

    def pack(step, carry):
        rows = k_rows[pl.ds(pl.multiple_of(step * req_local * pairs, 256), req_local * pairs), :].astype(jnp.bfloat16)
        send_k[pl.ds(step * req_local, req_local)] = rows.reshape(req_local, pairs, k_rows.shape[1])
        return carry

    lax.fori_loop(0, n_dev, pack, 0)

    def start_k(o):
        @pl.when(o != OWN)
        def _():
            k_copy(o, 0).start()

        k_copy(o, 1).start()

    start_k(jnp.int32(0))
    k_out[me] = send_k[pl.ds(me * req_local, req_local)]

    def produce(o, carry):
        slot = lax.rem(o, 2)
        load(o, slot).wait()
        norm_rows(o, slot, 0, pair_req)

        @pl.when(o + 2 < n_off)
        def _():
            load(o + 2, slot).start()

        @pl.when(o != OWN)
        def _():
            c_copy(o, 0).start()

        c_copy(o, 1).start()

        start_k(o)
        return carry

    lax.fori_loop(1, n_off, produce, 0)
    c_out[:, pl.ds(pl.multiple_of(first_pos, 32), seq_local), :] = send_c[OWN, pl.ds(core * req_local, req_local)]

    def clear(r, carry):
        top_out[r] = jnp.full(top_out.shape[1:], MASKED, jnp.float32)
        total_out[r] = jnp.zeros(total_out.shape[1:], jnp.float32)
        mixed_out[r] = jnp.zeros(mixed_out.shape[1:], jnp.float32)
        return carry

    lax.fori_loop(0, req_local, clear, 0)

    def arrived(o):
        @pl.when(o != OWN)
        def _():
            c_copy(o, 0).wait_recv()
            k_copy(o, 0).wait_recv()

        c_copy(o, 1).wait_recv()
        k_copy(o, 1).wait_recv()

    def attend(stage, carry):
        places = [table([pair[i] for pair in EARLY], stage) for i in range(2)]
        chips = [chip_at(me, side, place, -1) for place in places]
        for place in places:
            arrived(place)

        def some(step, carry):
            requests = [step * TOGETHER + i for i in range(TOGETHER)]
            queries = [jnp.concatenate([q_lat[r], q_rope[r], q_rope[r]], axis=1) for r in requests]
            lengths = [lens_s[0, me * req_local + r] for r in requests]
            states = [(top_out[r], total_out[r], mixed_out[r]) for r in requests]
            states = attend_stage(chips, lengths, queries, c_out, k_out, requests, seq_local, states)
            for r, state in zip(requests, states):
                top_out[r], total_out[r], mixed_out[r] = state
            return carry

        lax.fori_loop(0, req_local // TOGETHER, some, 0)
        return carry

    lax.fori_loop(0, len(EARLY), attend, 0)

    def sent(o, carry):
        for copy in (c_copy, k_copy):

            @pl.when(o != OWN)
            def _():
                copy(o, 0).wait_send()

            copy(o, 1).wait_send()
        return carry

    lax.fori_loop(0, n_off, sent, 0)
    for pair in LATE:
        for place in pair:
            for dc in range(CORES):
                k_copy(place, dc).wait_recv()
                c_copy(place, dc).wait_recv()


def finish_kernel(side, c_in, k_in, top, total, mixed, lens_v, q_lat, q_rope, c_cache, k_cache, o_lat, lens_s, turned, o_here, c_sem, k_sem, o_sem, lens_sem):
    me = lax.axis_index("x")
    n_req, seq, _ = c_in.shape
    seq_local = seq // (side * side * CORES)

    def c_copy(r):
        return pltpu.make_async_copy(c_in.at[r], c_cache.at[r], c_sem.at[r])

    def start(r, carry):
        c_copy(r).start()
        return carry

    lens_copy = pltpu.make_async_copy(lens_v, lens_s, lens_sem)
    lens_copy.start()
    lax.fori_loop(0, n_req, start, 0)

    k_copy = pltpu.make_async_copy(turned, k_cache, k_sem)
    rope = turned.shape[1]
    shape = (rope, 2 * rope)
    eye = (lax.broadcasted_iota(jnp.int32, shape, 0) == lax.rem(lax.broadcasted_iota(jnp.int32, shape, 1), rope)).astype(jnp.bfloat16)

    def turn(step, carry):
        requests = [step * 4 + i for i in range(4)]
        results = [lax.dot_general(eye, stack_keys(k_in[:, r]), NT, preferred_element_type=jnp.float32) for r in requests]
        for r, result in zip(requests, results):
            turned[r] = result.astype(jnp.bfloat16)
        return carry

    lax.fori_loop(0, n_req // 4, turn, 0)
    k_copy.start()
    lens_copy.wait()

    def some(step, carry):
        requests = [step * TOGETHER + i for i in range(TOGETHER)]
        queries = [jnp.concatenate([q_lat[r], q_rope[r], q_rope[r]], axis=1) for r in requests]
        lengths = [lens_s[0, me * n_req + r] for r in requests]
        states = [(top[r], total[r], mixed[r]) for r in requests]
        for pair in LATE:
            chips = [chip_at(me, side, place, -1) for place in pair]
            states = attend_stage(chips, lengths, queries, c_in, k_in, requests, seq_local, states)
        for r, (_, weights, values) in zip(requests, states):
            o_here[r] = (values / jnp.sum(weights, axis=-1, keepdims=True)).astype(jnp.bfloat16)
        return carry

    lax.fori_loop(0, n_req // TOGETHER, some, 0)
    o_copy = pltpu.make_async_copy(o_here, o_lat, o_sem)
    o_copy.start()

    def finish(r, carry):
        c_copy(r).wait()
        return carry

    lax.fori_loop(0, n_req, finish, 0)
    k_copy.wait()
    o_copy.wait()


def solution(mesh):
    seq_spec = P("dp", "x", None)
    req_spec = P(("dp", "x"), None, None)
    vmem = pl.BlockSpec(memory_space=pltpu.VMEM)
    anywhere = pl.BlockSpec(memory_space=pl.ANY)
    n_dev = mesh.shape["x"]
    side = math.isqrt(n_dev // CORES)

    def local_step(c_raw, k_raw, norm_gain, rope_cos, rope_sin, seq_lens, q_lat, q_rope):
        n_all, seq_local, width = c_raw.shape
        rope = k_raw.shape[-1]
        req_local, heads, _ = q_lat.shape
        seq = n_dev * seq_local
        pairs = seq_local // 2
        n_off = len(OFFSETS)
        lanes = 2 * CORES * seq_local
        lens_row = seq_lens.reshape(1, n_all)
        state = pltpu.VMEM((req_local, heads, lanes), jnp.float32)
        received = pl.pallas_call(
            functools.partial(exchange_kernel, side),
            out_shape=(
                pltpu.VMEM((req_local, seq, width), jnp.bfloat16),
                pltpu.VMEM((n_dev, req_local, pairs, 2 * rope), jnp.bfloat16),
                state,
                state,
                pltpu.VMEM((req_local, heads, width), jnp.float32),
                pltpu.VMEM((1, n_all), jnp.int32),
                pltpu.VMEM(q_lat.shape, jnp.bfloat16),
                pltpu.VMEM(q_rope.shape, jnp.bfloat16),
            ),
            in_specs=[anywhere] * 8,
            out_specs=(vmem,) * 8,
            scratch_shapes=[
                pltpu.SMEM((1, n_all), jnp.int32),
                pltpu.VMEM((width,), jnp.bfloat16),
                pltpu.VMEM(rope_cos.shape, jnp.float32),
                pltpu.VMEM(rope_sin.shape, jnp.float32),
                pltpu.VMEM((2, CORES * req_local, seq_local, width), jnp.bfloat16),
                pltpu.VMEM((n_off, CORES * req_local, seq_local, width), jnp.bfloat16),
                pltpu.VMEM((seq_local, rope, n_all), jnp.bfloat16),
                pltpu.VMEM((n_all * pairs, 2 * rope), jnp.float32),
                pltpu.VMEM((n_all, pairs, 2 * rope), jnp.bfloat16),
                pltpu.SemaphoreType.DMA((7,)),
                pltpu.SemaphoreType.DMA((CORES,)),
                pltpu.SemaphoreType.DMA((2,)),
                pltpu.SemaphoreType.DMA,
                pltpu.SemaphoreType.DMA((n_off, CORES)),
                pltpu.SemaphoreType.DMA((n_off, CORES)),
                pltpu.SemaphoreType.DMA((n_off, CORES)),
                pltpu.SemaphoreType.DMA((n_off, CORES)),
            ],
            compiler_params=pltpu.CompilerParams(collective_id=0, has_side_effects=True, vmem_limit_bytes=42 * MIB),
            name="exchange",
        )(lens_row, c_raw, jnp.transpose(k_raw, (1, 2, 0)), norm_gain, rope_cos, rope_sin, q_lat, q_rope)
        c_cache, k_turned, o_lat = pl.pallas_call(
            functools.partial(finish_kernel, side),
            out_shape=(
                jax.ShapeDtypeStruct((req_local, seq, width), jnp.bfloat16),
                jax.ShapeDtypeStruct((req_local, rope, seq), jnp.bfloat16),
                jax.ShapeDtypeStruct((req_local, heads, width), jnp.bfloat16),
            ),
            in_specs=[vmem] * 8,
            out_specs=(anywhere, anywhere, anywhere),
            scratch_shapes=[
                pltpu.SMEM((1, n_all), jnp.int32),
                pltpu.VMEM((req_local, rope, seq), jnp.bfloat16),
                pltpu.VMEM(q_lat.shape, jnp.bfloat16),
                pltpu.SemaphoreType.DMA((req_local,)),
                pltpu.SemaphoreType.DMA,
                pltpu.SemaphoreType.DMA,
                pltpu.SemaphoreType.DMA,
            ],
            compiler_params=pltpu.CompilerParams(vmem_limit_bytes=6 * MIB),
            name="finish",
        )(*received)
        return c_cache, jnp.transpose(k_turned, (0, 2, 1)), o_lat

    return jax.shard_map(local_step, mesh=mesh, in_specs=(seq_spec, seq_spec, P(None), P("x", None), P("x", None), P("dp"), req_spec, req_spec), out_specs=(req_spec, req_spec, req_spec), check_vma=False)
```

```python
import functools
import math

import jax
import jax.numpy as jnp
from jax import lax
from jax.experimental import pallas as pl
from jax.experimental.pallas import tpu as pltpu
from jax.sharding import PartitionSpec as P

NORM_EPS = 1e-6
MASKED = -1e30
MESH = pl.DeviceIdType.MESH
MIB = 2**20
CORES = 2
TOGETHER = 8
COPIED = 4

STAGES = (
    ((2, 2), (0, 0)),
    ((2, -1), (0, 1)),
    ((2, 1), (0, -1)),
    ((2, 0), (0, 2)),
    ((1, 2), (-1, 0)),
    ((-1, 2), (1, 0)),
    ((1, 1), (-1, -1)),
    ((1, -1), (-1, 1)),
)
OFFSETS = tuple(offset for stage in STAGES for offset in stage)
OWN = OFFSETS.index((0, 0))
EARLY = ((0, 1), (2, 3), (4, 5), (6, 7), (8, 9), (10, 11))
LATE = ((12, 13), (14, 15))
NT = (((1,), (1,)), ((), ()))


def table(values, index):
    if isinstance(index, int):
        return values[index]
    out = jnp.int32(values[0])
    for place, value in enumerate(values[1:], 1):
        out = jnp.where(index == place, jnp.int32(value), out)
    return out


def chip_at(me, side, place, sign=1):
    chip = me // CORES
    dx = table([(sign * dx) % side for dx, _ in OFFSETS], place)
    dy = table([(sign * dy) % side for _, dy in OFFSETS], place)
    return lax.rem(chip // side + dy, side) * side + lax.rem(lax.rem(chip, side) + dx, side)


def stack_keys(pairs_rows):
    lanes = pairs_rows.shape[-1]
    low = lax.broadcasted_iota(jnp.int32, (1, 1, lanes), 2) < lanes // 2
    zero = jnp.zeros_like(pairs_rows)
    split = [jnp.where(low, pairs_rows, zero)[:, None], jnp.where(low, zero, pairs_rows)[:, None]]
    return jnp.concatenate(split, axis=1).reshape(-1, lanes)


def attend_stage(chips, lengths, queries, c_ref, k_ref, requests, seq_local, states):
    span = CORES * seq_local
    starts = [pl.multiple_of(chip * span, span) for chip in chips]
    rows = [jnp.concatenate([c_ref[r, pl.ds(start, span), :] for start in starts], axis=0) for r in requests]
    keys = [jnp.concatenate([stack_keys(k_ref[pl.ds(chip * CORES, CORES), r]) for chip in chips], axis=0) for r in requests]
    scale = (rows[0].shape[-1] + keys[0].shape[-1] // 2) ** -0.5
    scores = [lax.dot_general(q, jnp.concatenate([row, key], axis=1), NT, preferred_element_type=jnp.float32) for q, row, key in zip(queries, rows, keys)]
    lane = lax.broadcasted_iota(jnp.int32, scores[0].shape, 1)
    position = jnp.where(lane < span, starts[0] + lane, starts[1] - span + lane)
    scores = [jnp.where(position < length, score * scale, MASKED) for score, length in zip(scores, lengths)]
    tops = [jnp.maximum(state[0], jnp.max(score, axis=-1, keepdims=True)) for state, score in zip(states, scores)]
    keeps = [jnp.exp(state[0] - top) for state, top in zip(states, tops)]
    weights = [jnp.exp(score - top) for score, top in zip(scores, tops)]
    added = [jnp.dot(weight.astype(jnp.bfloat16), row, preferred_element_type=jnp.float32) for weight, row in zip(weights, rows)]
    out = []
    for (_, total, mixed), top, keep, weight, add in zip(states, tops, keeps, weights, added):
        wide_keep = jnp.concatenate([keep] * (mixed.shape[-1] // keep.shape[-1]), axis=1)
        out.append((top, total * keep + weight, mixed * wide_keep + add))
    return out


def exchange_kernel(
    side, lens_h, c_raw, k_raw, gain_h, cos_h, sin_h, q_lat_h, q_rope_h,
    c_out, k_out, top_out, total_out, mixed_out, lens_v, q_lat, q_rope,
    lens_s, gain, cos, sin, raw, send_c, k_in, k_rows, send_k,
    small_sem, half_sem, raw_sem, k_sem, c_send, c_recv, k_send, k_recv,
):
    me = lax.axis_index("x")
    group = lax.axis_index("dp")
    core = lax.rem(me, CORES)
    n_dev = side * side * CORES
    n_off = len(OFFSETS)
    seq_local = c_raw.shape[1]
    req_local, heads, _ = q_lat.shape
    pair_req = CORES * req_local
    half = cos.shape[1]
    pairs = seq_local // 2
    first_pos = me * seq_local

    barrier = pltpu.get_barrier_semaphore()

    def greet(step, carry):
        pl.semaphore_signal(barrier, inc=1, device_id=(group, lax.rem(me + step, n_dev)), device_id_type=MESH)
        return carry

    def load(o, slot):
        return pltpu.make_async_copy(c_raw.at[pl.ds(chip_at(me, side, o) * pair_req, pair_req)], raw.at[slot], raw_sem.at[slot])

    def load_half(dc):
        there = lax.rem(core + dc, CORES) * req_local
        return pltpu.make_async_copy(c_raw.at[pl.ds(chip_at(me, side, 0) * pair_req + there, req_local)], raw.at[0, pl.ds(there, req_local)], half_sem.at[dc])

    def c_copy(o, dc):
        chip = chip_at(me, side, o)
        there = lax.rem(core + dc, CORES)
        return pltpu.make_async_remote_copy(
            send_c.at[o, pl.ds(there * req_local, req_local)],
            c_out.at[:, pl.ds(pl.multiple_of(first_pos, 32), seq_local), :],
            c_send.at[o, dc],
            c_recv.at[o, dc],
            device_id=(group, chip * CORES + there),
            device_id_type=MESH,
        )

    def k_copy(o, dc):
        chip = chip_at(me, side, o)
        there = lax.rem(core + dc, CORES)
        dest = chip * CORES + there
        return pltpu.make_async_remote_copy(
            send_k.at[pl.ds(dest * req_local, req_local)],
            k_out.at[me],
            k_send.at[o, dc],
            k_recv.at[o, dc],
            device_id=(group, dest),
            device_id_type=MESH,
        )

    def norm_rows(o, slot, start, count):
        first = chip_at(me, side, o) * pair_req
        scale = gain[...].astype(jnp.float32).reshape(1, gain.shape[0])

        def body(step, carry):
            row = start + step
            length = lens_s[0, first + row]
            x = raw[slot, row].astype(jnp.float32)
            inv = lax.rsqrt(jnp.mean(x * x, axis=-1, keepdims=True) + NORM_EPS)
            valid = first_pos + lax.broadcasted_iota(jnp.int32, inv.shape, 0) < length
            send_c[o, row] = jnp.where(valid, x * inv * scale, 0.0).astype(jnp.bfloat16)
            return carry

        lax.fori_loop(0, count, body, 0, unroll=4)

    small = [
        pltpu.make_async_copy(src, dst, small_sem.at[i])
        for i, (src, dst) in enumerate(((lens_h, lens_s), (gain_h, gain), (lens_h, lens_v), (cos_h, cos), (sin_h, sin), (q_lat_h, q_lat), (q_rope_h, q_rope)))
    ]
    k_load = pltpu.make_async_copy(k_raw, k_in, k_sem)
    load_half(0).start()
    small[0].start()
    small[1].start()
    lax.fori_loop(1, n_dev, greet, 0)
    load_half(1).start()
    load(1, 1).start()
    k_load.start()
    for copy in small[2:]:
        copy.start()
    small[0].wait()
    small[1].wait()
    load_half(0).wait()
    norm_rows(0, 0, core * req_local, req_local)
    pl.semaphore_wait(barrier, n_dev - 1)
    c_copy(0, 0).start()
    load_half(1).wait()
    norm_rows(0, 0, (CORES - 1 - core) * req_local, req_local)
    c_copy(0, 1).start()
    load(2, 0).start()

    for copy in small[2:]:
        copy.wait()
    k_load.wait()
    cos_t = cos[...].T
    sin_t = sin[...].T
    for pair in range(pairs):
        pieces = []
        for pos in (pair, pair + pairs):
            lo = k_in[pos, :half, :].astype(jnp.float32)
            hi = k_in[pos, half:, :].astype(jnp.float32)
            c = cos_t[:, pos : pos + 1]
            s = sin_t[:, pos : pos + 1]
            keep = first_pos + pos < lens_v[...]
            pieces.append(jnp.where(keep, lo * c - hi * s, 0.0))
            pieces.append(jnp.where(keep, hi * c + lo * s, 0.0))
        k_rows[pl.ds(pair, k_rows.shape[0] // pairs, stride=pairs), :] = jnp.concatenate(pieces, axis=0).T

    def pack(step, carry):
        rows = k_rows[pl.ds(pl.multiple_of(step * req_local * pairs, 256), req_local * pairs), :].astype(jnp.bfloat16)
        send_k[pl.ds(step * req_local, req_local)] = rows.reshape(req_local, pairs, k_rows.shape[1])
        return carry

    lax.fori_loop(0, n_dev, pack, 0)

    def start_k(o):
        @pl.when(o != OWN)
        def _():
            k_copy(o, 0).start()

        k_copy(o, 1).start()

    start_k(jnp.int32(0))
    k_out[me] = send_k[pl.ds(me * req_local, req_local)]

    def produce(o, carry):
        slot = lax.rem(o, 2)
        load(o, slot).wait()
        norm_rows(o, slot, 0, pair_req)

        @pl.when(o + 2 < n_off)
        def _():
            load(o + 2, slot).start()

        @pl.when(o != OWN)
        def _():
            c_copy(o, 0).start()

        c_copy(o, 1).start()

        start_k(o)
        return carry

    lax.fori_loop(1, n_off, produce, 0)
    c_out[:, pl.ds(pl.multiple_of(first_pos, 32), seq_local), :] = send_c[OWN, pl.ds(core * req_local, req_local)]

    def clear(r, carry):
        top_out[r] = jnp.full(top_out.shape[1:], MASKED, jnp.float32)
        total_out[r] = jnp.zeros(total_out.shape[1:], jnp.float32)
        mixed_out[r] = jnp.zeros(mixed_out.shape[1:], jnp.float32)
        return carry

    lax.fori_loop(0, req_local, clear, 0)

    def arrived(o):
        @pl.when(o != OWN)
        def _():
            c_copy(o, 0).wait_recv()
            k_copy(o, 0).wait_recv()

        c_copy(o, 1).wait_recv()
        k_copy(o, 1).wait_recv()

    def attend(stage, carry):
        places = [table([pair[i] for pair in EARLY], stage) for i in range(2)]
        chips = [chip_at(me, side, place, -1) for place in places]
        for place in places:
            arrived(place)

        def some(step, carry):
            requests = [step * TOGETHER + i for i in range(TOGETHER)]
            queries = [jnp.concatenate([q_lat[r], q_rope[r], q_rope[r]], axis=1) for r in requests]
            lengths = [lens_s[0, me * req_local + r] for r in requests]
            states = [(top_out[r], total_out[r], mixed_out[r]) for r in requests]
            states = attend_stage(chips, lengths, queries, c_out, k_out, requests, seq_local, states)
            for r, state in zip(requests, states):
                top_out[r], total_out[r], mixed_out[r] = state
            return carry

        lax.fori_loop(0, req_local // TOGETHER, some, 0)
        return carry

    lax.fori_loop(0, len(EARLY), attend, 0)

    def sent(o, carry):
        for copy in (c_copy, k_copy):

            @pl.when(o != OWN)
            def _():
                copy(o, 0).wait_send()

            copy(o, 1).wait_send()
        return carry

    lax.fori_loop(0, n_off, sent, 0)
    for pair in LATE:
        for place in pair:
            for dc in range(CORES):
                k_copy(place, dc).wait_recv()
                c_copy(place, dc).wait_recv()


def finish_kernel(side, c_in, k_in, top, total, mixed, lens_v, q_lat, q_rope, c_cache, k_cache, o_lat, lens_s, turned, o_here, c_sem, k_sem, o_sem, lens_sem):
    me = lax.axis_index("x")
    n_req, seq, _ = c_in.shape
    seq_local = seq // (side * side * CORES)

    def c_copy(r):
        some_requests = pl.ds(r * COPIED, COPIED)
        return pltpu.make_async_copy(c_in.at[some_requests], c_cache.at[some_requests], c_sem.at[r])

    def start(r, carry):
        c_copy(r).start()
        return carry

    lens_copy = pltpu.make_async_copy(lens_v, lens_s, lens_sem)
    lens_copy.start()
    lax.fori_loop(0, n_req // COPIED, start, 0)

    k_copy = pltpu.make_async_copy(turned, k_cache, k_sem)
    rope = turned.shape[1]
    shape = (rope, 2 * rope)
    eye = (lax.broadcasted_iota(jnp.int32, shape, 0) == lax.rem(lax.broadcasted_iota(jnp.int32, shape, 1), rope)).astype(jnp.bfloat16)

    def turn(step, carry):
        requests = [step * 4 + i for i in range(4)]
        results = [lax.dot_general(eye, stack_keys(k_in[:, r]), NT, preferred_element_type=jnp.float32) for r in requests]
        for r, result in zip(requests, results):
            turned[r] = result.astype(jnp.bfloat16)
        return carry

    lax.fori_loop(0, n_req // 4, turn, 0)
    k_copy.start()
    lens_copy.wait()

    def some(step, carry):
        requests = [step * TOGETHER + i for i in range(TOGETHER)]
        queries = [jnp.concatenate([q_lat[r], q_rope[r], q_rope[r]], axis=1) for r in requests]
        lengths = [lens_s[0, me * n_req + r] for r in requests]
        states = [(top[r], total[r], mixed[r]) for r in requests]
        for pair in LATE:
            chips = [chip_at(me, side, place, -1) for place in pair]
            states = attend_stage(chips, lengths, queries, c_in, k_in, requests, seq_local, states)
        for r, (_, weights, values) in zip(requests, states):
            o_here[r] = (values / jnp.sum(weights, axis=-1, keepdims=True)).astype(jnp.bfloat16)
        return carry

    lax.fori_loop(0, n_req // TOGETHER, some, 0)
    o_copy = pltpu.make_async_copy(o_here, o_lat, o_sem)
    o_copy.start()

    def finish(r, carry):
        c_copy(r).wait()
        return carry

    lax.fori_loop(0, n_req // COPIED, finish, 0)
    k_copy.wait()
    o_copy.wait()


def solution(mesh):
    seq_spec = P("dp", "x", None)
    req_spec = P(("dp", "x"), None, None)
    vmem = pl.BlockSpec(memory_space=pltpu.VMEM)
    anywhere = pl.BlockSpec(memory_space=pl.ANY)
    n_dev = mesh.shape["x"]
    side = math.isqrt(n_dev // CORES)

    def local_step(c_raw, k_raw, norm_gain, rope_cos, rope_sin, seq_lens, q_lat, q_rope):
        n_all, seq_local, width = c_raw.shape
        rope = k_raw.shape[-1]
        req_local, heads, _ = q_lat.shape
        seq = n_dev * seq_local
        pairs = seq_local // 2
        n_off = len(OFFSETS)
        lanes = 2 * CORES * seq_local
        lens_row = seq_lens.reshape(1, n_all)
        state = pltpu.VMEM((req_local, heads, lanes), jnp.float32)
        received = pl.pallas_call(
            functools.partial(exchange_kernel, side),
            out_shape=(
                pltpu.VMEM((req_local, seq, width), jnp.bfloat16),
                pltpu.VMEM((n_dev, req_local, pairs, 2 * rope), jnp.bfloat16),
                state,
                state,
                pltpu.VMEM((req_local, heads, width), jnp.float32),
                pltpu.VMEM((1, n_all), jnp.int32),
                pltpu.VMEM(q_lat.shape, jnp.bfloat16),
                pltpu.VMEM(q_rope.shape, jnp.bfloat16),
            ),
            in_specs=[anywhere] * 8,
            out_specs=(vmem,) * 8,
            scratch_shapes=[
                pltpu.SMEM((1, n_all), jnp.int32),
                pltpu.VMEM((width,), jnp.bfloat16),
                pltpu.VMEM(rope_cos.shape, jnp.float32),
                pltpu.VMEM(rope_sin.shape, jnp.float32),
                pltpu.VMEM((2, CORES * req_local, seq_local, width), jnp.bfloat16),
                pltpu.VMEM((n_off, CORES * req_local, seq_local, width), jnp.bfloat16),
                pltpu.VMEM((seq_local, rope, n_all), jnp.bfloat16),
                pltpu.VMEM((n_all * pairs, 2 * rope), jnp.float32),
                pltpu.VMEM((n_all, pairs, 2 * rope), jnp.bfloat16),
                pltpu.SemaphoreType.DMA((7,)),
                pltpu.SemaphoreType.DMA((CORES,)),
                pltpu.SemaphoreType.DMA((2,)),
                pltpu.SemaphoreType.DMA,
                pltpu.SemaphoreType.DMA((n_off, CORES)),
                pltpu.SemaphoreType.DMA((n_off, CORES)),
                pltpu.SemaphoreType.DMA((n_off, CORES)),
                pltpu.SemaphoreType.DMA((n_off, CORES)),
            ],
            compiler_params=pltpu.CompilerParams(collective_id=0, has_side_effects=True, vmem_limit_bytes=42 * MIB),
            name="exchange",
        )(lens_row, c_raw, jnp.transpose(k_raw, (1, 2, 0)), norm_gain, rope_cos, rope_sin, q_lat, q_rope)
        c_cache, k_turned, o_lat = pl.pallas_call(
            functools.partial(finish_kernel, side),
            out_shape=(
                jax.ShapeDtypeStruct((req_local, seq, width), jnp.bfloat16),
                jax.ShapeDtypeStruct((req_local, rope, seq), jnp.bfloat16),
                jax.ShapeDtypeStruct((req_local, heads, width), jnp.bfloat16),
            ),
            in_specs=[vmem] * 8,
            out_specs=(anywhere, anywhere, anywhere),
            scratch_shapes=[
                pltpu.SMEM((1, n_all), jnp.int32),
                pltpu.VMEM((req_local, rope, seq), jnp.bfloat16),
                pltpu.VMEM(q_lat.shape, jnp.bfloat16),
                pltpu.SemaphoreType.DMA((req_local // COPIED,)),
                pltpu.SemaphoreType.DMA,
                pltpu.SemaphoreType.DMA,
                pltpu.SemaphoreType.DMA,
            ],
            compiler_params=pltpu.CompilerParams(vmem_limit_bytes=6 * MIB),
            name="finish",
        )(*received)
        return c_cache, jnp.transpose(k_turned, (0, 2, 1)), o_lat

    return jax.shard_map(local_step, mesh=mesh, in_specs=(seq_spec, seq_spec, P(None), P("x", None), P("x", None), P("dp"), req_spec, req_spec), out_specs=(req_spec, req_spec, req_spec), check_vma=False)
```
